32 devices in a mesh: seq: 8 (over y, x, core), exp: 4 (over z).
Axes of the slice: x: 2, y: 2, z: 4, core: 2. Of those that a mesh axis runs over, the one named last changes fastest.
Arguments:
- grad_out: bfloat16 [4096, 2048], P(('seq', 'exp')), may hold values from -6 to 6
- out_proj: bfloat16 [4096, 2048], P('exp'), may hold values from -0.125 to 0.125
- step_size: float32 [64, 4096], P('exp', 'seq'), may hold values from 0.001 to 0.1
- log_decay: float32 [64, 4096], P('exp', 'seq'), may hold values from -1 to 0, as said below
- b_input: float32 [16, 4096], P(None, 'seq'), may hold values from -1.5 to 1.5
- c_output: float32 [16, 4096], P(None, 'seq'), may hold values from -1.5 to 1.5
- skip_gain: float32 [4096], P('exp'), may hold values from 0.5 to 1.5
- expert_ids: int32 [4096, 2], P('seq'), may hold values from 0 to 3, all different within a row; in each aligned block of 128 rows (0 to 127, 128 to 255, ...) at most 66 rows name the same one
- hidden_act: bfloat16 [4, 32, 66, 8192], P('exp', None, None, 'seq'), may hold values from -6 to 6
- w_down: bfloat16 [4, 8192, 2048], P('exp', 'seq'), may hold values from -0.0029296875 to 0.0029296875
Outputs:
- d_inner: bfloat16 [4096, 4096], P('seq', 'exp')
- d_gate: float32 [2, 4096], P(None, ('seq', 'exp'))
The draws below stay inside these ranges and needn't reach their ends.
Inputs may be any that keep to these rules, and one draw needn't show every extreme that they name: `expert_ids`: each row names 2 different experts. Within the rows of one token group no expert is named by more than 66 rows, and in every draw some expert is named by exactly 66 rows of some group. `log_decay`: every entry is negative.
All inputs are finite; a program needn't handle non-finite values.
Results may differ from the reference program's by a relative error of at most 0.00065.
Values may be sent and summed in bfloat16 or wider, within the bound.
A program may use at most 128 MiB of HBM per device.

```python
import math
from functools import partial
import jax
import jax.numpy as jnp
import numpy as np
from jax import lax

D = 2048
INNER = 4096
STATE = 16
HEAD = 64
FF = 8192
TOP = 2
TOK_DEV = 128
EXPERTS = 4
CAP = 66
SEQ_ROWS = 512
SEQUENCE_ITEMS = 4096
SOURCES = 32
HEADS = 64


def draw_log_decay(key, part):
    stochastic_seeds = jax.random.split(key, 7)
    slow_rate = jnp.exp(jax.random.uniform(stochastic_seeds[0], (HEADS, 1), jnp.float32, math.log(0.1 / SEQUENCE_ITEMS), math.log(0.8 / SEQUENCE_ITEMS)))
    fast_rate = jnp.exp(jax.random.uniform(stochastic_seeds[1], (HEADS, 1), jnp.float32, math.log(0.02), math.log(0.05)))
    slow_mask = jax.random.bernoulli(stochastic_seeds[2], 0.5, (HEADS, 1))
    per_channel_forgetting = jnp.where(slow_mask, slow_rate, fast_rate)
    forgetting_noise = jnp.exp(jax.random.uniform(stochastic_seeds[3], (HEADS, SEQUENCE_ITEMS), jnp.float32, math.log(0.5), math.log(2.0)))
    shard_draw = jnp.exp(jax.random.uniform(stochastic_seeds[4], (HEADS, SEQUENCE_ITEMS // SEQ_ROWS), jnp.float32, math.log(0.5), math.log(2.0)))
    shard_multiplier = jnp.repeat(shard_draw, SEQ_ROWS, axis=1)
    spike_opening_slot = jax.random.randint(stochastic_seeds[5], (2, 1), 0, SEQUENCE_ITEMS)
    spike_span = jax.random.uniform(stochastic_seeds[6], (2, 1), jnp.float32, 0.22, 0.45)
    sequence_offsets = lax.broadcasted_iota(jnp.int32, (2, SEQUENCE_ITEMS), 1)
    spike_table = jnp.sum(jnp.where(sequence_offsets == spike_opening_slot, spike_span, 0.0), axis=0)
    return -(per_channel_forgetting * forgetting_noise * shard_multiplier) - spike_table[None, :]


def level_of(rng, dims, shards, low, largest):
    gain = 1.0
    for dim, parts in shards:
        steps = jax.random.uniform(jax.random.fold_in(jax.random.fold_in(rng, 6), dim), (parts,), jnp.float32, low / len(shards), largest / len(shards))
        gain = gain * jnp.repeat(jnp.exp(steps), dims[dim] // parts).reshape((-1,) + (1,) * (len(dims) - 1 - dim))
    return gain


def assign_block(key, own, number, rows, amount, top, limit, skew):
    ranking = jax.random.permutation(key, amount)
    heavy_load, usual = shares(amount, rows * top, limit, skew, True), shares(amount, rows * top, limit, skew, False)
    places = jnp.arange(amount)

    def named(lengths, turn):
        used = int((lengths > 0).sum())
        fixed = max(1, used // 4)
        passed = fixed + (places - fixed + turn * (used - fixed)) % max(1, amount - fixed)
        return jnp.zeros((amount,), jnp.int32).at[ranking[jnp.where(places < fixed, places, passed)]].set(jnp.asarray(lengths, jnp.int32))

    lengths = jnp.where(number % 4 == 0, named(heavy_load, number // 4), named(usual, number - number // 4 - 1))
    mixed = jax.random.permutation(jax.random.fold_in(own, 3), amount)
    giver, taker = mixed[0:amount // 2 * 2:2], mixed[1:amount // 2 * 2:2]
    room = jnp.minimum(lengths[giver] - 1, limit - lengths[taker]) // 2
    room = jnp.where((giver == ranking[0]) | (taker == ranking[0]) | (lengths[taker] == 0), 0, jnp.maximum(room, 0))
    passed = jax.random.randint(jax.random.fold_in(own, 4), (amount // 2,), 0, 1 << 20) % (room + 1)
    lengths = lengths.at[giver].add(-passed).at[taker].add(passed)
    members = jnp.searchsorted(jnp.cumsum(lengths), jnp.arange(rows * top), side="right").astype(jnp.int32)
    table = members.reshape(top, rows).T
    table = table[jax.random.permutation(jax.random.fold_in(own, 1), rows)]
    turn = jax.random.randint(jax.random.fold_in(own, 2), (rows, 1), 0, top)
    return jnp.take_along_axis(table, (jnp.arange(top)[None, :] + turn) % top, axis=1)


def shares(amount, total, limit, slope, full):
    portions = [(1 << 20) // math.isqrt(standing ** slope) + 1 for standing in range(1, amount + 1)]
    largest = limit if full else min(limit, max(-(-total // amount), total * portions[0] // sum(portions)))
    least = 1 if total - largest >= amount - 1 else 0
    given, spare = [largest] + [least] * (amount - 1), total - largest - least * (amount - 1)
    while spare > 0:
        free = [i for i in range(1, amount) if given[i] < largest] or [i for i in range(1, amount) if given[i] < limit]
        mass, remaining = sum([portions[i] for i in free]), spare
        for i in free:
            more = min(limit - given[i], max(1, remaining * portions[i] // mass), spare)
            given[i] = given[i] + more
            spare = spare - more
    return np.array(given)


def normal_values(key, dims, width, bound, cuts=(), kind=jnp.bfloat16):
    entries = width * jax.random.normal(key, dims, jnp.float32)
    if cuts:
        entries = entries * level_of(key, dims, cuts, -0.22, 0.18)
    return jnp.clip(entries, -bound, bound).astype(kind)


def setup_inputs(seed: int = 0) -> dict:
    streams_of = jax.random.split(jax.random.key(seed), 11)
    grad_out = normal_values(streams_of[0], (SEQUENCE_ITEMS, D), 1.0, 6.0, ((0, 32),))
    out_proj = normal_values(streams_of[1], (INNER, D), D ** -0.5, 0.125, ((0, 4),))
    step_size = jnp.clip(jnp.exp(math.log(0.1) - 4.6051702 * jax.random.uniform(streams_of[2], (HEADS, SEQUENCE_ITEMS), jnp.float32) ** level_of(streams_of[2], (HEADS, SEQUENCE_ITEMS), ((0, 4), (1, 8)), -0.2, 0.2)), 0.001, 0.1)
    log_decay = draw_log_decay(jax.random.fold_in(streams_of[10], 71), 0)
    b_input = normal_values(streams_of[4], (STATE, SEQUENCE_ITEMS), 0.25, 1.5, ((1, 8),), jnp.float32)
    c_output = normal_values(streams_of[5], (STATE, SEQUENCE_ITEMS), 0.25, 1.5, ((1, 8),), jnp.float32)
    skip_gain = jnp.clip(0.5 + 1.0 * jax.random.uniform(streams_of[6], (INNER,), jnp.float32) ** level_of(streams_of[6], (INNER,), ((0, 4),), -0.2, 0.2), 0.5, 1.5)
    expert_ids_keys = jax.random.split(jax.random.fold_in(streams_of[7], 1), SEQUENCE_ITEMS // TOK_DEV)
    expert_ids_turns = jax.random.permutation(jax.random.fold_in(streams_of[7], 3), SEQUENCE_ITEMS // TOK_DEV)
    expert_ids = jax.vmap(lambda own, number: assign_block(jax.random.fold_in(streams_of[7], 2), own, number, TOK_DEV, EXPERTS, TOP, CAP, 0))(expert_ids_keys, expert_ids_turns).reshape((SEQUENCE_ITEMS, TOP))
    hidden_act = normal_values(streams_of[8], (EXPERTS, SOURCES, CAP, FF), 1.0, 6.0, ((0, 4), (3, 8)))
    w_down = normal_values(streams_of[9], (EXPERTS, FF, D), (FF * D // 4) ** -0.5, 0.0029296875, ((0, 4), (1, 8)))
    return {"grad_out": grad_out, "out_proj": out_proj, "step_size": step_size, "log_decay": log_decay, "b_input": b_input, "c_output": c_output, "skip_gain": skip_gain, "expert_ids": expert_ids, "hidden_act": hidden_act, "w_down": w_down}


highest = lax.Precision.HIGHEST


def block_pass(state_in, pieces):
    grad_block, decay_block, step_block, b_block, c_block = pieces
    cum_decay = jnp.cumsum(decay_block, axis=1)
    gap_table = cum_decay[:, None, :] - cum_decay[:, :, None]
    upper_mask = lax.broadcasted_iota(jnp.int32, gap_table.shape, 2) >= lax.broadcasted_iota(jnp.int32, gap_table.shape, 1)
    weights = jnp.where(upper_mask, jnp.exp(jnp.where(upper_mask, gap_table, 0.0)), 0.0)
    intersection = lax.dot_general(b_block, c_block, (((0,), (0,)), ((), ())), precision=highest, preferred_element_type=jnp.float32)
    within = jnp.einsum("hut,thp->uhp", weights * intersection[None], grad_block, precision=highest)
    tail_decay = jnp.exp(cum_decay[:, -1:] - cum_decay)
    from_state = jnp.einsum("nu,hnp->uhp", b_block, state_in, precision=highest) * tail_decay.T[:, :, None]
    result = step_block.T[:, :, None] * (within + from_state)
    state_out = jnp.einsum("ht,nt,thp->hnp", jnp.exp(cum_decay), c_block, grad_block, precision=highest)
    state_out = state_out + jnp.exp(cum_decay[:, -1])[:, None, None] * state_in
    return state_out, result


def local_sweep(grad_rows, decay_rows, step_rows, b_rows, c_rows, start_state):
    row_count = grad_rows.shape[0]
    head_count = decay_rows.shape[0]
    block_len = min(512, row_count)
    block_count = row_count // block_len
    pieces = (grad_rows.reshape(block_count, block_len, head_count, grad_rows.shape[2]),
              decay_rows.reshape(head_count, block_count, block_len).transpose(1, 0, 2),
              step_rows.reshape(head_count, block_count, block_len).transpose(1, 0, 2),
              b_rows.reshape(b_rows.shape[0], block_count, block_len).transpose(1, 0, 2),
              c_rows.reshape(c_rows.shape[0], block_count, block_len).transpose(1, 0, 2))
    state_out, results = lax.scan(block_pass, start_state, pieces, reverse=True)
    return state_out, results.reshape(row_count, head_count, grad_rows.shape[2])


def route_table(groups, expert, cap_len):
    hit_mask = jnp.any(groups == expert, axis=2)
    rank_ids = jnp.cumsum(hit_mask.astype(jnp.int32), axis=1) - 1
    slot_ids = lax.broadcasted_iota(jnp.int32, (1, 1, cap_len), 2)
    chosen = jnp.logical_and(hit_mask[:, :, None], rank_ids[:, :, None] == slot_ids)
    token_ids = lax.broadcasted_iota(jnp.int32, chosen.shape, 1)
    position = jnp.sum(jnp.where(chosen, token_ids, 0), axis=1).astype(jnp.int32)
    filled = jnp.any(chosen, axis=1)
    return position, filled


def slot_lookup(slot_table, own_ids, cap_len, expert_count):
    experts_iota = lax.broadcasted_iota(jnp.int32, (1, 1, expert_count), 2)
    onehot = own_ids[:, :, None] == experts_iota
    member = jnp.any(onehot, axis=1).astype(jnp.int32)
    rank_ids = jnp.cumsum(member, axis=0) - 1
    slot_of = jnp.sum(jnp.where(onehot, rank_ids[:, None, :], 0), axis=2)
    picked = jnp.sum(jnp.where(onehot[:, :, :, None], slot_table[None, None], 0.0), axis=2)
    slot_iota = lax.broadcasted_iota(jnp.int32, (1, 1, cap_len), 2)
    return jnp.sum(jnp.where(slot_of[:, :, None] == slot_iota, picked, 0.0), axis=2)


def reference(grad_out, out_proj, step_size, log_decay, b_input, c_output, skip_gain, expert_ids, hidden_act, w_down):
    inner_grad = jnp.dot(grad_out, out_proj.T, preferred_element_type=jnp.float32)
    start_state = jnp.zeros((HEADS, STATE, HEAD), jnp.float32)
    unused, swept_part = local_sweep(inner_grad.reshape(SEQUENCE_ITEMS, HEADS, HEAD), log_decay, step_size, b_input, c_output, start_state)
    d_inner = (swept_part.reshape(SEQUENCE_ITEMS, INNER) + skip_gain * inner_grad).astype(jnp.bfloat16)
    groups = expert_ids.reshape(SOURCES, TOK_DEV, TOP)
    sources = grad_out.reshape(SOURCES, TOK_DEV, D)

    def per_expert(pieces):
        expert, saved_part, weights = pieces
        position, filled = route_table(groups, expert, CAP)
        slot_rows = jnp.take_along_axis(sources, position[:, :, None], axis=1)
        slot_rows = jnp.where(filled[:, :, None], slot_rows, jnp.zeros_like(slot_rows))
        projected = jnp.dot(slot_rows.reshape(SOURCES * CAP, D), weights.T, preferred_element_type=jnp.float32)
        scores = jnp.sum(projected * saved_part.reshape(SOURCES * CAP, FF).astype(jnp.float32), axis=1)
        return scores.reshape(SOURCES, CAP)

    slot_scores = lax.map(per_expert, (jnp.arange(EXPERTS, dtype=jnp.int32), hidden_act, w_down))
    lookup = partial(slot_lookup, cap_len=CAP, expert_count=EXPERTS)
    values = jax.vmap(lookup, in_axes=(1, 0))(slot_scores, groups)
    d_gate = values.reshape(SEQUENCE_ITEMS, TOP).T
    return d_inner, d_gate
```

```python
import functools

import jax
import jax.numpy as jnp
from jax import lax
from jax.experimental import pallas as pl
from jax.experimental.pallas import tpu as pltpu
from jax.sharding import PartitionSpec as P

HEAD = 64


highest = lax.Precision.HIGHEST


def block_pass(state_in, pieces):
    grad_block, decay_block, step_block, b_block, c_block = pieces
    cum_decay = jnp.cumsum(decay_block, axis=1)
    gap_table = cum_decay[:, None, :] - cum_decay[:, :, None]
    upper_mask = lax.broadcasted_iota(jnp.int32, gap_table.shape, 2) >= lax.broadcasted_iota(
        jnp.int32, gap_table.shape, 1
    )
    weights = jnp.where(upper_mask, jnp.exp(jnp.where(upper_mask, gap_table, 0.0)), 0.0)
    intersection = lax.dot_general(
        b_block,
        c_block,
        (((0,), (0,)), ((), ())),
        precision=highest,
        preferred_element_type=jnp.float32,
    )
    within = jnp.einsum("hut,thp->uhp", weights * intersection[None], grad_block, precision=highest)
    tail_decay = jnp.exp(cum_decay[:, -1:] - cum_decay)
    from_state = (
        jnp.einsum("nu,hnp->uhp", b_block, state_in, precision=highest) * tail_decay.T[:, :, None]
    )
    result = step_block.T[:, :, None] * (within + from_state)
    state_out = jnp.einsum(
        "ht,nt,thp->hnp", jnp.exp(cum_decay), c_block, grad_block, precision=highest
    )
    state_out = state_out + jnp.exp(cum_decay[:, -1])[:, None, None] * state_in
    return (state_out, result)


def local_sweep(grad_rows, decay_rows, step_rows, b_rows, c_rows, start_state):
    row_count = grad_rows.shape[0]
    head_count = decay_rows.shape[0]
    block_len = min(512, row_count)
    block_count = row_count // block_len
    pieces = (
        grad_rows.reshape(block_count, block_len, head_count, grad_rows.shape[2]),
        decay_rows.reshape(head_count, block_count, block_len).transpose(1, 0, 2),
        step_rows.reshape(head_count, block_count, block_len).transpose(1, 0, 2),
        b_rows.reshape(b_rows.shape[0], block_count, block_len).transpose(1, 0, 2),
        c_rows.reshape(c_rows.shape[0], block_count, block_len).transpose(1, 0, 2),
    )
    state_out, results = lax.scan(block_pass, start_state, pieces, reverse=True)
    return (state_out, results.reshape(row_count, head_count, grad_rows.shape[2]))


def route_table(groups, expert, cap_len):
    hit_mask = jnp.any(groups == expert, axis=2)
    rank_ids = jnp.cumsum(hit_mask.astype(jnp.int32), axis=1) - 1
    slot_ids = lax.broadcasted_iota(jnp.int32, (1, 1, cap_len), 2)
    chosen = jnp.logical_and(hit_mask[:, :, None], rank_ids[:, :, None] == slot_ids)
    token_ids = lax.broadcasted_iota(jnp.int32, chosen.shape, 1)
    position = jnp.sum(jnp.where(chosen, token_ids, 0), axis=1)
    filled = jnp.any(chosen, axis=1)
    return (position, filled)


def slot_lookup(slot_table, own_ids, cap_len, expert_count):
    experts_iota = lax.broadcasted_iota(jnp.int32, (1, 1, expert_count), 2)
    onehot = own_ids[:, :, None] == experts_iota
    member = jnp.any(onehot, axis=1).astype(jnp.int32)
    rank_ids = jnp.cumsum(member, axis=0) - 1
    slot_of = jnp.sum(jnp.where(onehot, rank_ids[:, None, :], 0), axis=2)
    picked = jnp.sum(jnp.where(onehot[:, :, :, None], slot_table[None, None], 0.0), axis=2)
    slot_iota = lax.broadcasted_iota(jnp.int32, (1, 1, cap_len), 2)
    return jnp.sum(jnp.where(slot_of[:, :, None] == slot_iota, picked, 0.0), axis=2)


def shards(
    grad_out,
    out_proj,
    step_size,
    log_decay,
    b_input,
    c_output,
    skip_gain,
    expert_ids,
    hidden_act,
    w_down,
):
    exp_index = lax.axis_index("exp")
    seq_index = lax.axis_index("seq")
    exp_count = lax.axis_size("exp")
    seq_count = lax.axis_size("seq")
    tok_len = grad_out.shape[0]
    cap_len = hidden_act.shape[2]
    gathered = lax.all_gather(grad_out, "exp", axis=0, tiled=True)
    groups = expert_ids.reshape(exp_count, tok_len, expert_ids.shape[1])
    position, filled = route_table(groups, exp_index, cap_len)
    flat_index = (position + lax.broadcasted_iota(jnp.int32, position.shape, 0) * tok_len).reshape(
        -1
    )
    slot_rows = jnp.take(gathered, flat_index, axis=0)
    slot_rows = jnp.where(filled.reshape(-1, 1), slot_rows, jnp.zeros_like(slot_rows))
    saved_rows = hidden_act.reshape(-1, hidden_act.shape[3])
    weights = w_down[0]
    projected = lax.dot_general(
        lax.all_gather(slot_rows, "seq", axis=0, tiled=True),
        weights,
        (((1,), (1,)), ((), ())),
        preferred_element_type=jnp.float32,
    )
    partial_scores = jnp.sum(projected * saved_rows.astype(jnp.float32), axis=1)
    head_count = out_proj.shape[0] // HEAD
    inner_grad = lax.dot_general(
        gathered, out_proj, (((1,), (1,)), ((), ())), preferred_element_type=jnp.float32
    )
    row_count = inner_grad.shape[0]
    start_state = jnp.zeros((head_count, b_input.shape[0], HEAD), jnp.float32)
    summary, swept_part = local_sweep(
        inner_grad.reshape(row_count, head_count, HEAD),
        log_decay,
        step_size,
        b_input,
        c_output,
        start_state,
    )
    total_decay = jnp.sum(log_decay, axis=1)
    all_states, all_decay = (
        lax.all_gather(summary[None], "seq", axis=0, tiled=True),
        lax.all_gather(total_decay[None], "seq", axis=0, tiled=True),
    )
    shard_ids = lax.broadcasted_iota(jnp.int32, all_decay.shape, 0)
    beyond = jnp.where(shard_ids > seq_index, all_decay, 0.0)
    exponent = jnp.cumsum(beyond, axis=0) - beyond
    factor = jnp.where(
        shard_ids > seq_index, jnp.exp(jnp.where(shard_ids > seq_index, exponent, 0.0)), 0.0
    )
    incoming = jnp.sum(factor[:, :, None, None] * all_states, axis=0)
    suffix = jnp.flip(jnp.cumsum(jnp.flip(log_decay, 1), axis=1), 1) - log_decay
    from_carry = (
        jnp.einsum("nu,hnp->uhp", b_input, incoming, precision=highest)
        * jnp.exp(suffix).T[:, :, None]
    )
    combined = swept_part + step_size.T[:, :, None] * from_carry
    d_inner = (combined.reshape(row_count, -1) + skip_gain * inner_grad).astype(jnp.bfloat16)
    summed = lax.psum_scatter(
        partial_scores.reshape(seq_count, exp_count, cap_len),
        "seq",
        scatter_dimension=0,
        tiled=True,
    )
    slot_table = lax.all_to_all(
        summed.reshape(exp_count, 1, cap_len), "exp", split_axis=0, concat_axis=1, tiled=True
    ).reshape(exp_count, cap_len)
    own_ids = lax.dynamic_slice_in_dim(expert_ids, exp_index * tok_len, tok_len, 0)
    d_gate = slot_lookup(slot_table, own_ids, cap_len, exp_count).T
    return (d_inner, d_gate)


VMEM_ROOM = 63 << 20
BF = jnp.bfloat16
F32 = jnp.float32
LAG_FIRST = 2
LAG_SECOND = 4
scope = jax.named_scope


def halves(x):
    top = x.astype(BF)
    return top, (x - top.astype(F32)).astype(BF)


def dot(x, y, dims=((1,), (0,)), precision=None):
    return lax.dot_general(x, y, (dims, ((), ())), precision=precision, preferred_element_type=F32)


def flip(index, bit):
    return index + bit - 2 * bit * ((index // bit) % 2)


def column(table, h):
    lanes = lax.broadcasted_iota(jnp.int32, table.shape, 1)
    return jnp.sum(jnp.where(lanes == h, table, 0.0), axis=1, keepdims=True)


def nearest(z, i):
    upper = z // 2
    low = z + upper * (3 - 2 * z)
    group = i + low * (1 - i // 2) * (1 - 2 * i)
    return group + upper * (3 - 2 * group)


def turn_of(z, group):
    upper = z // 2
    low = z + upper * (3 - 2 * z)
    mirrored = group + upper * (3 - 2 * group)
    return mirrored + low * (1 - mirrored // 2) * (1 - 2 * mirrored)


def fused(
    sizes,
    grad_hbm, proj_hbm, hid_hbm, down_hbm, step_ref, decay_ref, b_ref, c_ref, skip_ref, ids_ref,
    out_ref, gate_ref,
    gath, proj, hid, down, turned, y_ref, y_tail, rows, tail, pick, pick_tail, inner, fac, fac_mid,
    acc, acc_tail, cum_ref, cum_t, step_t, b_t, bc, mix, lead, mid, span_sum, span_got, agg, got,
    carry, spot, mail, inbox, vals,
    load_sem, hid_sem, down_sem, proj_sem,
    zs_sem, zr_sem, xs_sem, xr_sem, ds_sem, dr_sem, as_sem, ar_sem, ms_sem, mr_sem,
):
    n_seq, n_exp, tok, cap, parts, width = sizes
    me = lax.axis_index("seq")
    z = lax.axis_index("exp")
    row_count = n_exp * tok
    n_dev = n_seq * n_exp
    mine_id = me * n_exp + z
    bits = [1 << i for i in range(1, n_seq.bit_length() - 1)]
    order = [1] + bits
    n_stage = len(bits)
    block = bc.shape[1]
    blocks = row_count // block
    channels = inner.shape[1]
    lane = 2 * HEAD
    pairs = channels // lane
    main = y_ref.shape[2]
    extra = cap - main
    half_w = width // 2
    units = n_exp * parts
    n_state = b_t.shape[1]

    for k in range(parts):
        pltpu.make_async_copy(
            grad_hbm.at[:, pl.ds(k * width, width)], gath.at[k, z], load_sem.at[k]
        ).start()
    hid_copy = pltpu.make_async_copy(hid_hbm.at[0], hid, hid_sem)
    hid_copy.start()
    for k in range(parts):
        pltpu.make_async_copy(
            down_hbm.at[0, :, pl.ds(k * width, width)], down.at[k], down_sem.at[k]
        ).start()
    for k in range(parts):
        pltpu.make_async_copy(
            proj_hbm.at[:, pl.ds(k * width, width)], proj.at[k], proj_sem.at[k]
        ).start()

    barrier = pltpu.get_barrier_semaphore()

    def greet(i, _):
        other = lax.rem(mine_id + i, n_dev)
        pl.semaphore_signal(
            barrier, inc=1, device_id={"seq": other // n_exp, "exp": lax.rem(other, n_exp)}
        )
        return 0

    with scope("greet"):
        lax.fori_loop(1, n_dev, greet, 0)

    with scope("prep"):
        hit = jnp.zeros((1, row_count), F32)
        for i in range(ids_ref.shape[0]):
            hit = jnp.maximum(hit, jnp.where(ids_ref[i : i + 1, :] == z, 1.0, 0.0))
        row_id = lax.broadcasted_iota(jnp.int32, (row_count, row_count), 0)
        col_id = lax.broadcasted_iota(jnp.int32, (row_count, row_count), 1)
        same = jnp.logical_and(row_id // tok == col_id // tok, row_id < col_id)
        before = dot(
            jnp.broadcast_to(hit, (16, row_count)).astype(BF), jnp.where(same, 1.0, 0.0).astype(BF)
        )
        rank = before[0:1].astype(jnp.int32)
        group = lax.broadcasted_iota(jnp.int32, (1, row_count), 1) // tok
        place = jnp.where(hit > 0.5, rank, -1)
        slots = lax.broadcasted_iota(jnp.int32, (main, tok), 0)
        for g in range(n_exp):
            chosen = slots == place[:, g * tok : (g + 1) * tok]
            pick[g] = jnp.where(chosen, 1.0, 0.0).astype(BF)
        over = jnp.where(place >= main, (place - main) * n_exp + group, -1)
        chosen = lax.broadcasted_iota(jnp.int32, (16, row_count), 0) == over
        pick_tail[...] = jnp.where(chosen, 1.0, 0.0).astype(BF)

    with scope("barrier"):
        pl.semaphore_wait(barrier, n_dev - 1)

    def z_copy(side, k, d, owner, target):
        return pltpu.make_async_remote_copy(
            src_ref=gath.at[k, owner],
            dst_ref=gath.at[k, owner],
            send_sem=zs_sem.at[side, k, d],
            recv_sem=zr_sem.at[side, k, d],
            device_id={"exp": target},
        )

    def z_send(k, d):
        @pl.when(jnp.logical_and(z < n_exp - 1, z - d >= 0))
        def _():
            z_copy(0, k, d, z - d, z + 1).start()

        @pl.when(jnp.logical_and(z > 0, z + d < n_exp))
        def _():
            z_copy(1, k, d, z + d, z - 1).start()

    def z_sent(k, d):
        @pl.when(jnp.logical_and(z < n_exp - 1, z - d >= 0))
        def _():
            z_copy(0, k, d, z - d, z + 1).wait_send()

        @pl.when(jnp.logical_and(z > 0, z + d < n_exp))
        def _():
            z_copy(1, k, d, z + d, z - 1).wait_send()

    def z_take(k, d):
        @pl.when(z - d >= 0)
        def _():
            z_copy(0, k, d - 1, z - d, z).wait_recv()

        @pl.when(z + d < n_exp)
        def _():
            z_copy(1, k, d - 1, z + d, z).wait_recv()

    with scope("own"):
        for k in range(parts):
            pltpu.make_async_copy(
                grad_hbm.at[:, pl.ds(k * width, width)], gath.at[k, z], load_sem.at[k]
            ).wait()
            z_send(k, 0)

    def bit_of(half, stage):
        if stage == n_stage:
            return 1
        return bits[stage] if half == 0 else bits[n_stage - 1 - stage]

    def x_copies(u, stage, here):
        masks = [()]
        for i in range(stage):
            masks = masks + [m + (i,) for m in masks]
        copies = []
        for j, mask in enumerate(masks):
            for half in range(2):
                owner = me
                for i in mask:
                    owner = flip(owner, bit_of(half, i))
                slot = (1 << stage) - 1 + j
                if not here:
                    owner = flip(owner, bit_of(half, stage))
                if u is None:
                    index, ref = 2 * units + half, tail.at[half, owner]
                else:
                    index, ref = 2 * u + half, rows.at[2 * u + half, owner]
                copies.append(pltpu.make_async_remote_copy(
                    src_ref=ref,
                    dst_ref=ref,
                    send_sem=xs_sem.at[index, slot],
                    recv_sem=xr_sem.at[index, slot],
                    device_id={"seq": flip(me, bit_of(half, stage))},
                ))
        return copies

    def x_start(u, stage):
        for mine in x_copies(u, stage, True):
            mine.start()

    def x_take(u, stage):
        for theirs in x_copies(u, stage, False):
            theirs.wait_recv()

    def x_pass(u, stage):
        x_take(u, stage - 1)
        x_start(u, stage)

    def x_sent(u):
        for stage in range(n_stage + 1):
            for mine in x_copies(u, stage, True):
                mine.wait_send()

    def d_copy(i):
        return pltpu.make_async_remote_copy(
            src_ref=span_sum.at[i],
            dst_ref=span_got.at[i],
            send_sem=ds_sem.at[i],
            recv_sem=dr_sem.at[i],
            device_id={"seq": flip(me, order[i])},
        )

    def settle():
        own = pl.multiple_of(z * tok, tok)
        named = [ids_ref[k : k + 1, pl.ds(own, tok)] for k in range(ids_ref.shape[0])]
        expert = lax.broadcasted_iota(jnp.int32, (16, tok), 0)
        member = jnp.zeros((16, tok), F32)
        for ids in named:
            member = jnp.maximum(member, jnp.where(ids == expert, 1.0, 0.0))
        earlier = lax.broadcasted_iota(jnp.int32, (tok, tok), 0) < lax.broadcasted_iota(
            jnp.int32, (tok, tok), 1
        )
        ranks = dot(member.astype(BF), jnp.where(earlier, 1.0, 0.0).astype(BF)).astype(jnp.int32)
        for k, ids in enumerate(named):
            slot = jnp.zeros((1, tok), jnp.int32)
            shift = jnp.zeros((1, tok), jnp.int32)
            for e in range(n_exp):
                slot += jnp.where(ids == e, ranks[e : e + 1], 0)
                shift += jnp.where(ids == e, (turn_of(e, z) % 2) * main, 0)
            far = (me // 2) * 16 + (slot - main) * 2 * n_exp + (me % 2) * n_exp + z
            spot[k : k + 1, :] = jnp.where(slot < main, shift + slot, far)
            spot[2 + k : 3 + k, :] = ids * 2 + jnp.where(slot < main, 0, 1)

    def prepare():
        row_id = lax.broadcasted_iota(jnp.int32, (row_count, row_count), 0)
        col_id = lax.broadcasted_iota(jnp.int32, (row_count, row_count), 1)
        tri = jnp.where(row_id <= col_id, 1.0, 0.0)
        cum = dot(decay_ref[...], tri, precision=highest)
        cum_ref[...] = cum
        cum_t[...] = jnp.transpose(cum)
        step_t[...] = jnp.transpose(step_ref[...])
        b_t[...] = jnp.transpose(b_ref[...])
        shape = (cum.shape[0], channels)
        own = lax.broadcasted_iota(jnp.int32, shape, 1) // HEAD == lax.broadcasted_iota(
            jnp.int32, shape, 0
        )
        end = jnp.sum(jnp.where(own, cum[:, row_count - 1 :], 0.0), axis=0, keepdims=True)
        span_sum[0] = jnp.broadcast_to(end, (8, channels))
        keep = lax.broadcasted_iota(jnp.int32, (block, block), 1) >= lax.broadcasted_iota(
            jnp.int32, (block, block), 0
        )
        for i in range(blocks):
            span = slice(i * block, (i + 1) * block)
            cross = dot(b_t[span, :], c_ref[:, span], precision=highest)
            bc[i] = jnp.where(keep, cross, 0.0)
        acc[...] = jnp.zeros_like(acc)
        acc_tail[...] = jnp.zeros_like(acc_tail)

    left_of = lax.broadcasted_iota(jnp.int32, (1, lane), 1) < HEAD
    perm_row = lax.broadcasted_iota(jnp.int32, (256, 256), 0)
    perm_col = lax.broadcasted_iota(jnp.int32, (256, 256), 1)

    def project(job):
        b, n = job // parts, job % parts
        q_first = pl.multiple_of((b % 2) * 16, 16)
        c_first = (b // 2) * 32

        @pl.when(n == 0)
        def _():
            swap = jnp.where(perm_col == (perm_row % 16) * 16 + perm_row // 16, 1.0, 0.0).astype(BF)
            for i in range(2):
                saved = hid[pl.ds(c_first + 16 * i, 16), pl.ds(q_first, 16), :]
                saved = saved.reshape(256, hid.shape[2])
                turned[256 * i : 256 * (i + 1), :] = dot(swap, saved).astype(BF)

        part = dot(turned[...], down[n])
        for i in range(2):
            y_ref[n, pl.ds(q_first, 16), pl.ds(pl.multiple_of(c_first + 16 * i, 16), 16), :] = part[
                256 * i : 256 * (i + 1)
            ].reshape(16, 16, width)

    def hoist(j):
        span = pl.ds(pl.multiple_of(j * lane, lane), lane)
        cols = [column(cum_t[...], 2 * j + i) for i in range(2)]
        rowv = [cum_ref[pl.ds(2 * j + i, 1), :] for i in range(2)]
        steps = [column(step_t[...], 2 * j + i) for i in range(2)]
        steps_col = jnp.where(left_of, steps[0], steps[1])
        col = jnp.where(left_of, cols[0], cols[1])
        end_row = jnp.where(left_of, cols[0][row_count - 1 :], cols[1][row_count - 1 :])
        fac[:, span] = steps_col * jnp.exp(end_row - col)
        for i in range(blocks):
            lo, hi = i * block, (i + 1) * block
            if i < blocks - 1:
                fac_mid[lo:hi, span] = steps_col[lo:hi] * jnp.exp(col[hi - 1 : hi] - col[lo:hi])
            for q in range(2):
                r = rowv[q][:, lo:hi]
                w = jnp.exp(jnp.minimum(r - cols[q][lo:hi], 0.0)) * (bc[i] * steps[q][lo:hi])
                w_top, w_low = halves(w)
                mix[j, i, q * block : (q + 1) * block, :] = w_top
                mix[j, i, (2 + q) * block : (3 + q) * block, :] = w_low
                base = rowv[q][:, lo - 1 : lo] if i else jnp.zeros((1, 1), F32)
                m_top, m_low = halves(c_ref[:, lo:hi] * jnp.exp(r - base))
                lead[j, i, q * n_state : (q + 1) * n_state, :] = m_top
                lead[j, i, (2 + q) * n_state : (3 + q) * n_state, :] = m_low

    def state_step(j, _):
        span = pl.ds(pl.multiple_of(j * lane, lane), lane)
        rowv = [cum_ref[pl.ds(2 * j + q, 1), :] for q in range(2)]
        ends = [[r[:, hi - 1 : hi] for r in rowv] for hi in range(block, row_count + 1, block)]
        state = jnp.zeros((n_state, lane), F32)
        for i in reversed(range(blocks)):
            g_top, g_low = halves(inner[i * block : (i + 1) * block, span])
            x = dot(lead[j, i], jnp.concatenate([g_top, g_low], axis=1))
            x = x[:, :lane] + jnp.concatenate(
                [x[: 2 * n_state, lane:], jnp.zeros((2 * n_state, lane), F32)], axis=0
            )
            x = x[: 2 * n_state] + x[2 * n_state :]
            if i < blocks - 1:
                mid[i, :, span] = state
            edge = jnp.where(left_of, ends[i][0], ends[i][1])
            if i:
                edge = edge - jnp.where(left_of, ends[i - 1][0], ends[i - 1][1])
            state = jnp.where(left_of, x[:n_state], x[n_state:]) + jnp.exp(edge) * state
        agg[0, :, span] = state
        return 0

    def within_step(j, _):
        span = pl.ds(pl.multiple_of(j * lane, lane), lane)
        skip = skip_ref[:, span]
        for i in range(blocks):
            lo, hi = i * block, (i + 1) * block
            g = inner[lo:hi, span]
            g_top, g_low = halves(g)
            x = dot(mix[j, i], jnp.concatenate([g_top, g_low], axis=1))
            part = []
            for q in range(2):
                top = x[q * block : (q + 1) * block]
                low = x[(2 + q) * block : (3 + q) * block]
                part.append(top[:, :lane] + top[:, lane:] + low[:, :lane])
            result = jnp.where(left_of, part[0], part[1]) + skip * g
            if i < blocks - 1:
                seen = dot(b_t[lo:hi, :], mid[i, :, span], precision=highest)
                result += fac_mid[lo:hi, span] * seen
            inner[lo:hi, span] = result
        return 0

    def scores(u):
        i, c = u // parts, u % parts
        g = nearest(z, i)

        def one(s, _):
            total = acc[s, i]
            for half in range(2):
                part = rows[2 * u + half, s].astype(F32) * y_ref[
                    c, s * n_exp + g, :, half * half_w : (half + 1) * half_w
                ]
                for j in range(half_w // 128):
                    total = total + part[:, j * 128 : (j + 1) * 128]
            acc[s, i] = total
            return 0

        lax.fori_loop(0, n_seq, one, 0)

    low_half = lax.broadcasted_iota(jnp.int32, (2 * n_exp, width), 0) < n_exp

    def tail_scores():
        def one(p, _):
            sums = [acc_tail[p, i] for i in range(extra)]
            for c in range(parts):
                half, at = c // 2, (c % 2) * width
                first = tail[half, 2 * p].astype(F32)[: 2 * n_exp, at : at + width]
                second = tail[half, 2 * p + 1].astype(F32)[: 2 * n_exp, at : at + width]
                even = jnp.where(low_half, first, pltpu.roll(second, n_exp, 0))
                odd = jnp.where(low_half, pltpu.roll(first, n_exp, 0), second)
                for i, part in enumerate((even, odd)):
                    first_q = pl.multiple_of(p * 2 * n_exp, 2 * n_exp)
                    part = part * y_tail[c, i, pl.ds(first_q, 2 * n_exp), :]
                    for j in range(width // 128):
                        sums[i] = sums[i] + part[:, j * 128 : (j + 1) * 128]
            for i in range(extra):
                acc_tail[p, i] = sums[i]
            return 0

        lax.fori_loop(0, n_seq // 2, one, 0)

    def unit_step(t, _):
        i, c = t // parts, t % parts

        with scope("ztake"):
            @pl.when(i >= 1)
            def _():
                z_take(c, i)

            @pl.when(jnp.logical_and(i >= 1, i < n_exp - 1))
            def _():
                z_send(c, i)

        g = nearest(z, i)
        with scope("pick"):
            taken = dot(pick[g], gath[c, g]).astype(BF)
            rows[2 * t, me] = taken[:, :half_w]
            rows[2 * t + 1, me] = taken[:, half_w:]
            x_start(t, 0)

        with scope("xpass1"):
            @pl.when(t >= LAG_FIRST)
            def _():
                x_pass(t - LAG_FIRST, 1)

        with scope("xpass2"):
            @pl.when(t >= LAG_SECOND)
            def _():
                x_pass(t - LAG_SECOND, 2)

        with scope("once"):
            @pl.when(t == 0)
            def _():
                prepare()
                d_copy(0).start()
                settle()
                hid_copy.wait()

            for k in range(parts):
                @pl.when(t == k)
                def _(k=k):
                    pltpu.make_async_copy(
                        down_hbm.at[0, :, pl.ds(k * width, width)], down.at[k], down_sem.at[k]
                    ).wait()
                    pltpu.make_async_copy(
                        proj_hbm.at[:, pl.ds(k * width, width)], proj.at[k], proj_sem.at[k]
                    ).wait()

            for i_ in range(len(order)):
                @pl.when(t == 2 * i_ + 3)
                def _(i_=i_):
                    d_copy(i_).wait_recv()
                    if i_ + 1 < len(order):
                        span_sum[i_ + 1] = span_sum[i_] + span_got[i_]
                        d_copy(i_ + 1).start()

        with scope("project"):
            @pl.when(jnp.logical_and(t >= parts - 1, t < 3 * parts - 1))
            def _():
                project(2 * (t - parts + 1))
                project(2 * (t - parts + 1) + 1)

            @pl.when(jnp.logical_and(t >= 2 * parts, t < 3 * parts))
            def _():
                saved = hid[main:cap].reshape(extra * hid.shape[1], hid.shape[2])
                y_tail[c] = dot(saved, down[c]).reshape(extra, hid.shape[1], width)

        with scope("inner"):
            @pl.when(i % 2 == 1)
            def _():
                other = nearest(z, i - 1)
                both = jnp.concatenate([gath[c, other], gath[c, g]], axis=0)
                part = dot(both, proj[c], ((1,), (1,)))
                first = pl.ds(pl.multiple_of(other * tok, tok), tok)
                second = pl.ds(pl.multiple_of(g * tok, tok), tok)

                @pl.when(c == 0)
                def _():
                    inner[first, :] = part[:tok]
                    inner[second, :] = part[tok:]

                @pl.when(c > 0)
                def _():
                    inner[first, :] += part[:tok]
                    inner[second, :] += part[tok:]

        with scope("hoist"):
            @pl.when(jnp.logical_and(t >= units - pairs, t < units))
            def _():
                hoist(t - (units - pairs))

        with scope("tailrows"):
            @pl.when(i == n_exp - 1)
            def _():
                left = dot(pick_tail[...], gath[c].reshape(row_count, width)).astype(BF)
                tail[c // 2, me, :, pl.ds(pl.multiple_of((c % 2) * width, width), width)] = left

        with scope("score"):
            @pl.when(t >= 3 * parts)
            def _():
                for v in range(2):
                    u = 2 * (t - 3 * parts) + v
                    x_take(u, n_stage)
                    scores(u)

        return 0

    with scope("unitloop"):
        lax.fori_loop(0, units, unit_step, 0)

    def a_copy(i):
        return pltpu.make_async_remote_copy(
            src_ref=agg.at[i],
            dst_ref=got.at[i],
            send_sem=as_sem.at[i],
            recv_sem=ar_sem.at[i],
            device_id={"seq": flip(me, order[i])},
        )

    reach = [jnp.zeros((1, channels), F32)]

    def combine(i):
        a_copy(i).wait_recv()
        low = ((me // order[i]) % 2) == 0
        other, other_t = got[i], span_got[i, 0:1, :]
        own, own_t = agg[i], span_sum[i, 0:1, :]
        added = jnp.where(low, jnp.exp(reach[0]) * other, 0.0)
        if i == 0:
            carry[...] = added
        else:
            carry[...] += added
        reach[0] = reach[0] + jnp.where(low, other_t, 0.0)
        if i + 1 < len(order):
            first = jnp.where(low, own, other)
            first_t = jnp.where(low, own_t, other_t)
            second = jnp.where(low, other, own)
            agg[i + 1] = first + jnp.exp(first_t) * second
            a_copy(i + 1).start()

    def mail_copy(other, source, slot):
        return pltpu.make_async_remote_copy(
            src_ref=mail.at[other // n_exp, turn_of(z, lax.rem(other, n_exp)) // 2],
            dst_ref=inbox.at[source],
            send_sem=ms_sem.at[slot],
            recv_sem=mr_sem.at[source],
            device_id={"seq": other // n_exp, "exp": lax.rem(other, n_exp)},
        )

    def post(i, _):
        other = lax.rem(mine_id + i, n_dev)
        mail_copy(other, mine_id, other).start()
        return 0

    def take(i, _):
        other = lax.rem(mine_id + i, n_dev)
        mail_copy(other, other, other).wait_recv()
        return 0

    def posted(i, _):
        other = lax.rem(mine_id + i, n_dev)
        mail_copy(other, mine_id, other).wait_send()
        return 0

    done = [2 * parts]

    def pace(stage):
        with scope("p%d" % stage):
            if stage == 0:
                x_start(None, 0)
                x_pass(units - 2, 1)
            if stage == 1:
                x_pass(units - 4, 2)
                x_pass(units - 1, 1)
                x_pass(None, 1)
            if stage == 2:
                x_pass(units - 3, 2)
            if stage == 3:
                x_pass(units - 2, 2)
            if stage == 4:
                x_pass(units - 1, 2)
                x_pass(None, 2)

    def count(upto):
        with scope("c%d" % upto):
            for u in range(done[0], upto):
                x_take(u, n_stage)
                scores(u)
            done[0] = max(done[0], upto)

    pace(0)
    with scope("state"):
        lax.fori_loop(0, pairs, state_step, 0)
        a_copy(0).start()
    pace(1)
    with scope("within1"):
        lax.fori_loop(0, pairs // 4, within_step, 0)
    pace(2)
    with scope("comb0"):
        combine(0)
    count(units - 4)
    pace(3)
    with scope("within2"):
        lax.fori_loop(pairs // 4, pairs // 2, within_step, 0)
    pace(4)
    with scope("comb1"):
        combine(1)
    count(units)
    with scope("tailscore"):
        x_take(None, n_stage)
        tail_scores()

    with scope("finish"):
        wide = jnp.transpose(acc_tail[...].reshape(n_seq // 2 * extra * 2 * n_exp, 128))
        wide = jnp.sum(wide, axis=0, keepdims=True)
        wide = jnp.concatenate([wide, jnp.zeros((1, 128 - wide.shape[1]), F32)], axis=1)

        def finish(s, _):
            for i in range(n_exp // 2):
                both = jnp.transpose(acc[s, 2 * i : 2 * i + 2].reshape(2 * main, 128))
                mail[s, i, 0:1, :] = jnp.sum(both, axis=0, keepdims=True)
                mail[s, i, 1:2, :] = wide
            return 0

        lax.fori_loop(0, n_seq, finish, 0)
    with scope("post"):
        lax.fori_loop(1, n_dev, post, 0)
        inbox[mine_id] = mail[me, 0]

    with scope("within3"):
        lax.fori_loop(pairs // 2, pairs, within_step, 0)
    with scope("comb2"):
        combine(2)
    with scope("out"):
        for i in range(blocks):
            lo, hi = i * block, (i + 1) * block
            from_carry = dot(b_t[lo:hi, :], carry[...], precision=highest)
            out_ref[lo:hi, :] = (inner[lo:hi, :] + fac[lo:hi, :] * from_carry).astype(BF)

    with scope("drain"):
        def x_drain(u, _):
            x_sent(u)
            return 0

        lax.fori_loop(0, units, x_drain, 0)
        x_sent(None)
        for k in range(parts):
            for d in range(n_exp - 1):
                z_sent(k, d)
        for i in range(len(order)):
            a_copy(i).wait_send()
            d_copy(i).wait_send()
    with scope("mail"):
        lax.fori_loop(1, n_dev, take, 0)
    with scope("gate"):
        for e in range(n_exp):
            total = inbox[e]
            for i in range(1, n_seq):
                total = total + inbox[i * n_exp + e]
            vals[2 * e : 2 * e + 2, :] = total
        for k in range(ids_ref.shape[0]):
            at = lax.broadcasted_iota(jnp.int32, (128, tok), 0) == spot[k : k + 1, :]
            found = dot(vals[...], jnp.where(at, 1.0, 0.0), precision=highest)
            pickd = lax.broadcasted_iota(jnp.int32, (2 * n_exp, tok), 0) == spot[2 + k : 3 + k, :]
            gate_ref[k : k + 1, :] = jnp.sum(jnp.where(pickd, found, 0.0), axis=0, keepdims=True)
        lax.fori_loop(1, n_dev, posted, 0)


def plan(n_seq, n_exp, tok, depth, channels, cap, hidden, state, top):
    parts = 4
    width = depth // parts
    main = cap // 16 * 16
    extra = cap - main
    row_count = n_exp * tok
    block = min(256, row_count)
    blocks = row_count // block
    heads = channels // HEAD
    pairs = heads // 2
    stages = n_seq.bit_length() - 1
    steps = n_exp - 1
    units = n_exp * parts
    groups = n_seq * n_exp
    shapes = [
        ((parts, n_exp, tok, width), BF),
        ((parts, channels, width), BF),
        ((cap, groups, hidden), BF),
        ((parts, hidden, width), BF),
        ((512, hidden), BF),
        ((parts, groups, main, width), F32),
        ((parts, extra, groups, width), F32),
        ((2 * units, n_seq, main, width // 2), BF),
        ((2, n_seq, 16, depth // 2), BF),
        ((n_exp, main, tok), BF),
        ((16, row_count), BF),
        ((row_count, channels), F32),
        ((row_count, channels), F32),
        ((max(row_count - block, 8), channels), F32),
        ((n_seq, n_exp, main, 128), F32),
        ((n_seq // 2, extra, 2 * n_exp, 128), F32),
        ((heads, row_count), F32),
        ((row_count, heads), F32),
        ((row_count, heads), F32),
        ((row_count, state), F32),
        ((blocks, block, block), F32),
        ((pairs, blocks, 4 * block, block), BF),
        ((pairs, blocks, 4 * state, block), BF),
        ((max(blocks - 1, 1), state, channels), F32),
        ((stages, 8, channels), F32),
        ((stages, 8, channels), F32),
        ((stages, state, channels), F32),
        ((stages, state, channels), F32),
        ((state, channels), F32),
        ((8, tok), jnp.int32),
        ((n_seq, n_exp // 2, 2, 128), F32),
        ((groups, 2, 128), F32),
        ((2 * n_exp, 128), F32),
    ]
    total = 0
    for shape, kind in shapes:
        size = 1
        for extent in shape:
            size *= extent
        total += size * (2 if kind is BF else 4)
    fits = (
        total < VMEM_ROOM - (4 << 20)
        and n_seq & (n_seq - 1) == 0
        and stages == 3
        and n_exp == 4
        and groups == 32
        and main == 64
        and extra == 2
        and top == 2
        and depth % (256 * parts) == 0
        and channels % (2 * HEAD) == 0
        and pairs <= units // 2
        and row_count % block == 0
        and tok == 128
    )
    sems = [
        (parts,), (), (parts,), (parts,),
        (2, parts, steps), (2, parts, steps),
        (2 * units + 2, n_seq - 1), (2 * units + 2, n_seq - 1),
        (stages,), (stages,), (stages,), (stages,),
        (groups,), (groups,),
    ]
    return fits, (n_seq, n_exp, tok, cap, parts, width), shapes, sems


def quick(
    fitted, grad_out, out_proj, step_size, log_decay, b_input, c_output, skip_gain, expert_ids,
    hidden_act, w_down,
):
    _, sizes, shapes, sems = fitted
    n_seq, n_exp, tok, cap, parts, width = sizes
    vmem = pl.BlockSpec(memory_space=pltpu.VMEM)
    hbm = pl.BlockSpec(memory_space=pl.ANY)
    row_count, channels = n_exp * tok, out_proj.shape[0]
    return pl.pallas_call(
        functools.partial(fused, sizes),
        out_shape=(
            jax.ShapeDtypeStruct((row_count, channels), BF),
            jax.ShapeDtypeStruct((expert_ids.shape[1], tok), F32),
        ),
        in_specs=[hbm] * 4 + [vmem] * 6,
        out_specs=(vmem, vmem),
        scratch_shapes=[pltpu.VMEM(shape, kind) for shape, kind in shapes]
        + [pltpu.SemaphoreType.DMA(s) if s else pltpu.SemaphoreType.DMA for s in sems],
        compiler_params=pltpu.CompilerParams(
            collective_id=0, has_side_effects=True, vmem_limit_bytes=VMEM_ROOM
        ),
    )(
        grad_out, out_proj, hidden_act.transpose(0, 2, 1, 3), w_down, step_size, log_decay, b_input, c_output,
        skip_gain.reshape(1, -1), expert_ids.T,
    )


def route(*args):
    grad_out, out_proj, step_size, log_decay, b_input, c_output, skip_gain, ids, hidden, down = args
    fitted = plan(
        lax.axis_size("seq"), lax.axis_size("exp"), grad_out.shape[0], grad_out.shape[1],
        out_proj.shape[0], hidden.shape[2], hidden.shape[3], b_input.shape[0], ids.shape[1],
    )
    if fitted[0]:
        return quick(fitted, *args)
    return shards(*args)


def solution(mesh):
    in_specs = (
        P(("seq", "exp"), None),
        P("exp", None),
        P("exp", "seq"),
        P("exp", "seq"),
        P(None, "seq"),
        P(None, "seq"),
        P("exp"),
        P("seq", None),
        P("exp", None, None, "seq"),
        P("exp", "seq", None),
    )
    out_specs = (P("seq", "exp"), P(None, ("seq", "exp")))
    return jax.shard_map(route, mesh=mesh, in_specs=in_specs, out_specs=out_specs, check_vma=False)
```

```python
import functools

import jax
import jax.numpy as jnp
from jax import lax
from jax.experimental import pallas as pl
from jax.experimental.pallas import tpu as pltpu
from jax.sharding import PartitionSpec as P

HEAD = 64


highest = lax.Precision.HIGHEST


def block_pass(state_in, pieces):
    grad_block, decay_block, step_block, b_block, c_block = pieces
    cum_decay = jnp.cumsum(decay_block, axis=1)
    gap_table = cum_decay[:, None, :] - cum_decay[:, :, None]
    upper_mask = lax.broadcasted_iota(jnp.int32, gap_table.shape, 2) >= lax.broadcasted_iota(
        jnp.int32, gap_table.shape, 1
    )
    weights = jnp.where(upper_mask, jnp.exp(jnp.where(upper_mask, gap_table, 0.0)), 0.0)
    intersection = lax.dot_general(
        b_block,
        c_block,
        (((0,), (0,)), ((), ())),
        precision=highest,
        preferred_element_type=jnp.float32,
    )
    within = jnp.einsum("hut,thp->uhp", weights * intersection[None], grad_block, precision=highest)
    tail_decay = jnp.exp(cum_decay[:, -1:] - cum_decay)
    from_state = (
        jnp.einsum("nu,hnp->uhp", b_block, state_in, precision=highest) * tail_decay.T[:, :, None]
    )
    result = step_block.T[:, :, None] * (within + from_state)
    state_out = jnp.einsum(
        "ht,nt,thp->hnp", jnp.exp(cum_decay), c_block, grad_block, precision=highest
    )
    state_out = state_out + jnp.exp(cum_decay[:, -1])[:, None, None] * state_in
    return (state_out, result)


def local_sweep(grad_rows, decay_rows, step_rows, b_rows, c_rows, start_state):
    row_count = grad_rows.shape[0]
    head_count = decay_rows.shape[0]
    block_len = min(512, row_count)
    block_count = row_count // block_len
    pieces = (
        grad_rows.reshape(block_count, block_len, head_count, grad_rows.shape[2]),
        decay_rows.reshape(head_count, block_count, block_len).transpose(1, 0, 2),
        step_rows.reshape(head_count, block_count, block_len).transpose(1, 0, 2),
        b_rows.reshape(b_rows.shape[0], block_count, block_len).transpose(1, 0, 2),
        c_rows.reshape(c_rows.shape[0], block_count, block_len).transpose(1, 0, 2),
    )
    state_out, results = lax.scan(block_pass, start_state, pieces, reverse=True)
    return (state_out, results.reshape(row_count, head_count, grad_rows.shape[2]))


def route_table(groups, expert, cap_len):
    hit_mask = jnp.any(groups == expert, axis=2)
    rank_ids = jnp.cumsum(hit_mask.astype(jnp.int32), axis=1) - 1
    slot_ids = lax.broadcasted_iota(jnp.int32, (1, 1, cap_len), 2)
    chosen = jnp.logical_and(hit_mask[:, :, None], rank_ids[:, :, None] == slot_ids)
    token_ids = lax.broadcasted_iota(jnp.int32, chosen.shape, 1)
    position = jnp.sum(jnp.where(chosen, token_ids, 0), axis=1)
    filled = jnp.any(chosen, axis=1)
    return (position, filled)


def slot_lookup(slot_table, own_ids, cap_len, expert_count):
    experts_iota = lax.broadcasted_iota(jnp.int32, (1, 1, expert_count), 2)
    onehot = own_ids[:, :, None] == experts_iota
    member = jnp.any(onehot, axis=1).astype(jnp.int32)
    rank_ids = jnp.cumsum(member, axis=0) - 1
    slot_of = jnp.sum(jnp.where(onehot, rank_ids[:, None, :], 0), axis=2)
    picked = jnp.sum(jnp.where(onehot[:, :, :, None], slot_table[None, None], 0.0), axis=2)
    slot_iota = lax.broadcasted_iota(jnp.int32, (1, 1, cap_len), 2)
    return jnp.sum(jnp.where(slot_of[:, :, None] == slot_iota, picked, 0.0), axis=2)


def shards(
    grad_out,
    out_proj,
    step_size,
    log_decay,
    b_input,
    c_output,
    skip_gain,
    expert_ids,
    hidden_act,
    w_down,
):
    exp_index = lax.axis_index("exp")
    seq_index = lax.axis_index("seq")
    exp_count = lax.axis_size("exp")
    seq_count = lax.axis_size("seq")
    tok_len = grad_out.shape[0]
    cap_len = hidden_act.shape[2]
    gathered = lax.all_gather(grad_out, "exp", axis=0, tiled=True)
    groups = expert_ids.reshape(exp_count, tok_len, expert_ids.shape[1])
    position, filled = route_table(groups, exp_index, cap_len)
    flat_index = (position + lax.broadcasted_iota(jnp.int32, position.shape, 0) * tok_len).reshape(
        -1
    )
    slot_rows = jnp.take(gathered, flat_index, axis=0)
    slot_rows = jnp.where(filled.reshape(-1, 1), slot_rows, jnp.zeros_like(slot_rows))
    saved_rows = hidden_act.reshape(-1, hidden_act.shape[3])
    weights = w_down[0]
    projected = lax.dot_general(
        lax.all_gather(slot_rows, "seq", axis=0, tiled=True),
        weights,
        (((1,), (1,)), ((), ())),
        preferred_element_type=jnp.float32,
    )
    partial_scores = jnp.sum(projected * saved_rows.astype(jnp.float32), axis=1)
    head_count = out_proj.shape[0] // HEAD
    inner_grad = lax.dot_general(
        gathered, out_proj, (((1,), (1,)), ((), ())), preferred_element_type=jnp.float32
    )
    row_count = inner_grad.shape[0]
    start_state = jnp.zeros((head_count, b_input.shape[0], HEAD), jnp.float32)
    summary, swept_part = local_sweep(
        inner_grad.reshape(row_count, head_count, HEAD),
        log_decay,
        step_size,
        b_input,
        c_output,
        start_state,
    )
    total_decay = jnp.sum(log_decay, axis=1)
    all_states, all_decay = (
        lax.all_gather(summary[None], "seq", axis=0, tiled=True),
        lax.all_gather(total_decay[None], "seq", axis=0, tiled=True),
    )
    shard_ids = lax.broadcasted_iota(jnp.int32, all_decay.shape, 0)
    beyond = jnp.where(shard_ids > seq_index, all_decay, 0.0)
    exponent = jnp.cumsum(beyond, axis=0) - beyond
    factor = jnp.where(
        shard_ids > seq_index, jnp.exp(jnp.where(shard_ids > seq_index, exponent, 0.0)), 0.0
    )
    incoming = jnp.sum(factor[:, :, None, None] * all_states, axis=0)
    suffix = jnp.flip(jnp.cumsum(jnp.flip(log_decay, 1), axis=1), 1) - log_decay
    from_carry = (
        jnp.einsum("nu,hnp->uhp", b_input, incoming, precision=highest)
        * jnp.exp(suffix).T[:, :, None]
    )
    combined = swept_part + step_size.T[:, :, None] * from_carry
    d_inner = (combined.reshape(row_count, -1) + skip_gain * inner_grad).astype(jnp.bfloat16)
    summed = lax.psum_scatter(
        partial_scores.reshape(seq_count, exp_count, cap_len),
        "seq",
        scatter_dimension=0,
        tiled=True,
    )
    slot_table = lax.all_to_all(
        summed.reshape(exp_count, 1, cap_len), "exp", split_axis=0, concat_axis=1, tiled=True
    ).reshape(exp_count, cap_len)
    own_ids = lax.dynamic_slice_in_dim(expert_ids, exp_index * tok_len, tok_len, 0)
    d_gate = slot_lookup(slot_table, own_ids, cap_len, exp_count).T
    return (d_inner, d_gate)


VMEM_ROOM = 63 << 20
BF = jnp.bfloat16
F32 = jnp.float32
LAG_FIRST = 1
LAG_SECOND = 3
FIRST_STEPS = {
    0: ((0, 1),),
    1: ((1, 1), (2, 1)),
    2: ((3, 1), (0, 2)),
    3: ((1, 2),),
    4: ((2, 2),),
    5: ((3, 2),),
}
scope = jax.named_scope


def halves(x):
    top = x.astype(BF)
    return top, (x - top.astype(F32)).astype(BF)


def dot(x, y, dims=((1,), (0,)), precision=None):
    return lax.dot_general(x, y, (dims, ((), ())), precision=precision, preferred_element_type=F32)


def flip(index, bit):
    return index + bit - 2 * bit * ((index // bit) % 2)


def column(table, h):
    lanes = lax.broadcasted_iota(jnp.int32, table.shape, 1)
    return jnp.sum(jnp.where(lanes == h, table, 0.0), axis=1, keepdims=True)


def nearest(z, i):
    upper = z // 2
    low = z + upper * (3 - 2 * z)
    group = i + low * (1 - i // 2) * (1 - 2 * i)
    return group + upper * (3 - 2 * group)


def turn_of(z, group):
    upper = z // 2
    low = z + upper * (3 - 2 * z)
    mirrored = group + upper * (3 - 2 * group)
    return mirrored + low * (1 - mirrored // 2) * (1 - 2 * mirrored)


def fused(
    sizes,
    grad_hbm, proj_hbm, hid_hbm, down_hbm, step_hbm, decay_hbm, b_hbm, c_hbm, skip_hbm, ids_hbm,
    out_hbm, gate_ref,
    gath, proj, hid, down, turned, y_ref, y_tail, rows, tail, pick, pick_tail, inner, fac, fac_mid,
    acc, acc_tail, cum_ref, cum_t, step_t, b_t, bc, mix, lead, mid, span_sum, span_got, agg, got,
    carry, spot, mail, inbox, vals, out_buf, where_at, step_ref, decay_ref, b_ref, c_ref, skip_ref, ids_ref, b_wide,
    load_sem,
    zs_sem, zr_sem, xs_sem, xr_sem, ds_sem, dr_sem, as_sem, ar_sem, ms_sem, mr_sem, out_sem,
):
    n_seq, n_exp, tok, cap, parts, width = sizes
    me = lax.axis_index("seq")
    z = lax.axis_index("exp")
    row_count = n_exp * tok
    n_dev = n_seq * n_exp
    mine_id = me * n_exp + z
    bits = [1 << i for i in range(1, n_seq.bit_length() - 1)]
    order = [1] + bits
    n_stage = len(bits)
    block = bc.shape[1]
    blocks = row_count // block
    channels = inner.shape[1]
    lane = 2 * HEAD
    pairs = channels // lane
    main = y_ref.shape[2]
    extra = cap - main
    half_w = width // 2
    units = n_exp * parts
    n_state = b_t.shape[1]

    def load(k):
        return pltpu.make_async_copy(
            grad_hbm.at[:, pl.ds(k * width, width)], gath.at[k, z], load_sem.at[0]
        )

    def down_load(k):
        return pltpu.make_async_copy(
            down_hbm.at[0, :, pl.ds(k * width, width)], down.at[k], load_sem.at[1]
        )

    def proj_load(k):
        return pltpu.make_async_copy(
            proj_hbm.at[:, pl.ds(k * width, width)], proj.at[k], load_sem.at[2]
        )

    hid_copy = pltpu.make_async_copy(hid_hbm.at[0], hid, load_sem.at[3])
    ids_copy = pltpu.make_async_copy(ids_hbm, ids_ref, load_sem.at[4])
    small = [
        pltpu.make_async_copy(src, dst, load_sem.at[5 + i])
        for i, (src, dst) in enumerate((
            (step_hbm, step_ref), (decay_hbm, decay_ref), (b_hbm, b_ref), (c_hbm, c_ref),
            (skip_hbm, skip_ref),
        ))
    ]
    barrier = pltpu.get_barrier_semaphore()

    with scope("greet"):
        for bit in order:
            pl.semaphore_signal(barrier, inc=1, device_id={"seq": flip(me, bit)})

        @pl.when(z > 0)
        def _():
            pl.semaphore_signal(barrier, inc=1, device_id={"exp": z - 1})

        @pl.when(z < n_exp - 1)
        def _():
            pl.semaphore_signal(barrier, inc=1, device_id={"exp": z + 1})

    with scope("prep"):
        for k in range(parts):
            load(k).start()
        ids_copy.start()
        for copy in small:
            copy.start()
        ids_copy.wait()
        hit = jnp.zeros((1, row_count), F32)
        for i in range(ids_ref.shape[0]):
            hit = jnp.maximum(hit, jnp.where(ids_ref[i : i + 1, :] == z, 1.0, 0.0))
        row_id = lax.broadcasted_iota(jnp.int32, (row_count, row_count), 0)
        col_id = lax.broadcasted_iota(jnp.int32, (row_count, row_count), 1)
        same = jnp.logical_and(row_id // tok == col_id // tok, row_id < col_id)
        before = dot(
            jnp.broadcast_to(hit, (16, row_count)).astype(BF), jnp.where(same, 1.0, 0.0).astype(BF)
        )
        rank = before[0:1].astype(jnp.int32)
        group = lax.broadcasted_iota(jnp.int32, (1, row_count), 1) // tok
        place = jnp.where(hit > 0.5, rank, -1)
        slots = lax.broadcasted_iota(jnp.int32, (main, tok), 0)
        for g in range(n_exp):
            chosen = slots == place[:, g * tok : (g + 1) * tok]
            pick[g] = jnp.where(chosen, 1.0, 0.0).astype(BF)
        over = jnp.where(place >= main, (place - main) * n_exp + group, -1)
        chosen = lax.broadcasted_iota(jnp.int32, (16, row_count), 0) == over
        pick_tail[...] = jnp.where(chosen, 1.0, 0.0).astype(BF)

    with scope("barrier"):
        sides = jnp.minimum(z, 1) + jnp.minimum(n_exp - 1 - z, 1)
        pl.semaphore_wait(barrier, len(order) + sides)

    def z_copy(side, k, d, owner, target):
        return pltpu.make_async_remote_copy(
            src_ref=gath.at[k, owner],
            dst_ref=gath.at[k, owner],
            send_sem=zs_sem.at[side, d],
            recv_sem=zr_sem.at[side, k, d],
            device_id={"exp": target},
        )

    def z_send(k, d):
        @pl.when(jnp.logical_and(z < n_exp - 1, z - d >= 0))
        def _():
            z_copy(0, k, d, z - d, z + 1).start()

        @pl.when(jnp.logical_and(z > 0, z + d < n_exp))
        def _():
            z_copy(1, k, d, z + d, z - 1).start()

    def settled(ref, sem):
        pltpu.make_async_copy(ref, ref, sem).wait()

    def z_sent(d):
        @pl.when(jnp.logical_and(z < n_exp - 1, z - d >= 0))
        def _():
            settled(gath.at[:, z], zs_sem.at[0, d])

        @pl.when(jnp.logical_and(z > 0, z + d < n_exp))
        def _():
            settled(gath.at[:, z], zs_sem.at[1, d])

    def z_take(k, d):
        @pl.when(z - d >= 0)
        def _():
            z_copy(0, k, d - 1, z - d, z).wait_recv()

        @pl.when(z + d < n_exp)
        def _():
            z_copy(1, k, d - 1, z + d, z).wait_recv()

    with scope("own"):
        settled(gath.at[:, z], load_sem.at[0])
        for k in range(parts):
            z_send(k, 0)

    def bit_of(half, stage):
        if stage == n_stage:
            return 1
        return bits[stage] if half == 0 else bits[n_stage - 1 - stage]

    def owners(half, stage):
        held = [me]
        for i in range(stage):
            held = held + [flip(owner, bit_of(half, i)) for owner in held]
        return held

    def x_start(u, stage):
        for j in range(1 << stage):
            for half in range(2):
                ref = rows.at[2 * u + half, owners(half, stage)[j]]
                pltpu.make_async_remote_copy(
                    src_ref=ref,
                    dst_ref=ref,
                    send_sem=xs_sem.at[0],
                    recv_sem=xr_sem.at[u, stage],
                    device_id={"seq": flip(me, bit_of(half, stage))},
                ).start()

    def x_take(u, stage):
        settled(rows.at[pl.ds(2 * u, 2), pl.ds(0, 1 << stage)], xr_sem.at[u, stage])

    def x_pass(u, stage):
        x_take(u, stage - 1)
        x_start(u, stage)

    def t_start(half, stage):
        for owner in owners(half, stage):
            ref = tail.at[half, owner]
            pltpu.make_async_remote_copy(
                src_ref=ref,
                dst_ref=ref,
                send_sem=xs_sem.at[1],
                recv_sem=xr_sem.at[units + half, stage],
                device_id={"seq": flip(me, bit_of(half, stage))},
            ).start()

    def t_take(half, stage):
        settled(tail.at[half, pl.ds(0, 1 << stage)], xr_sem.at[units + half, stage])

    def t_pass(half, stage):
        t_take(half, stage - 1)
        t_start(half, stage)

    def d_copy(i):
        return pltpu.make_async_remote_copy(
            src_ref=span_sum.at[i],
            dst_ref=span_got.at[i],
            send_sem=ds_sem,
            recv_sem=dr_sem.at[i],
            device_id={"seq": flip(me, order[i])},
        )

    def settle():
        own = pl.multiple_of(z * tok, tok)
        named = [ids_ref[k : k + 1, pl.ds(own, tok)] for k in range(ids_ref.shape[0])]
        expert = lax.broadcasted_iota(jnp.int32, (16, tok), 0)
        member = jnp.zeros((16, tok), F32)
        for ids in named:
            member = jnp.maximum(member, jnp.where(ids == expert, 1.0, 0.0))
        earlier = lax.broadcasted_iota(jnp.int32, (tok, tok), 0) < lax.broadcasted_iota(
            jnp.int32, (tok, tok), 1
        )
        ranks = dot(member.astype(BF), jnp.where(earlier, 1.0, 0.0).astype(BF)).astype(jnp.int32)
        for k, ids in enumerate(named):
            slot = jnp.zeros((1, tok), jnp.int32)
            shift = jnp.zeros((1, tok), jnp.int32)
            for e in range(n_exp):
                slot += jnp.where(ids == e, ranks[e : e + 1], 0)
                shift += jnp.where(ids == e, (turn_of(e, z) % 2) * main, 0)
            far = (me // 2) * 16 + (slot - main) * 2 * n_exp + (me % 2) * n_exp + z
            at = lax.broadcasted_iota(jnp.int32, (128, tok), 0) == jnp.where(
                slot < main, shift + slot, far
            )
            where_at[:, k * tok : (k + 1) * tok] = jnp.where(at, 1.0, 0.0).astype(BF)
            spot[k : k + 1, :] = ids * 2 + jnp.where(slot < main, 0, 1)

    def prepare():
        for copy in small:
            copy.wait()
        row_id = lax.broadcasted_iota(jnp.int32, (row_count, row_count), 0)
        col_id = lax.broadcasted_iota(jnp.int32, (row_count, row_count), 1)
        tri = jnp.where(row_id <= col_id, 1.0, 0.0)
        cum = dot(decay_ref[...], tri, precision=highest)
        cum_ref[...] = cum
        cum_t[...] = jnp.transpose(cum)
        step_t[...] = jnp.transpose(step_ref[...])
        b_t[...] = jnp.transpose(b_ref[...])
        b_top, b_low = halves(b_t[...])
        b_wide[...] = jnp.concatenate([b_top, b_top, b_low], axis=1)
        shape = (cum.shape[0], channels)
        own = lax.broadcasted_iota(jnp.int32, shape, 1) // HEAD == lax.broadcasted_iota(
            jnp.int32, shape, 0
        )
        end = jnp.sum(jnp.where(own, cum[:, row_count - 1 :], 0.0), axis=0, keepdims=True)
        span_sum[0] = jnp.broadcast_to(end, (8, channels))
        keep = lax.broadcasted_iota(jnp.int32, (block, block), 1) >= lax.broadcasted_iota(
            jnp.int32, (block, block), 0
        )
        for i in range(blocks):
            span = slice(i * block, (i + 1) * block)
            cross = dot(b_t[span, :], c_ref[:, span], precision=highest)
            bc[i] = jnp.where(keep, cross, 0.0)
        acc[...] = jnp.zeros_like(acc)
        acc_tail[...] = jnp.zeros_like(acc_tail)

    left_of = lax.broadcasted_iota(jnp.int32, (1, lane), 1) < HEAD
    perm_row = lax.broadcasted_iota(jnp.int32, (256, 256), 0)
    perm_col = lax.broadcasted_iota(jnp.int32, (256, 256), 1)

    jobs = parts * main * hid.shape[1] // 512

    def project(job):
        b, n = job // parts, job % parts
        q_first = pl.multiple_of((b % 2) * 16, 16)
        c_first = (b // 2) * 32

        @pl.when(n == 0)
        def _():
            swap = jnp.where(perm_col == (perm_row % 16) * 16 + perm_row // 16, 1.0, 0.0).astype(BF)
            for i in range(2):
                saved = hid[pl.ds(c_first + 16 * i, 16), pl.ds(q_first, 16), :]
                saved = saved.reshape(256, hid.shape[2])
                turned[256 * i : 256 * (i + 1), :] = dot(swap, saved).astype(BF)

            @pl.when(b == jobs // parts - 1)
            def _():
                turned[512:, :] = hid[main:cap].reshape(extra * hid.shape[1], hid.shape[2])

        def keep_part(part):
            for i in range(2):
                c_from = pl.multiple_of(c_first + 16 * i, 16)
                y_ref[n, pl.ds(q_first, 16), pl.ds(c_from, 16), :] = part[
                    256 * i : 256 * (i + 1)
                ].reshape(16, 16, width)

        @pl.when(b < jobs // parts - 1)
        def _():
            keep_part(dot(turned[:512, :], down[n]))

        @pl.when(b == jobs // parts - 1)
        def _():
            part = dot(turned[...], down[n])
            keep_part(part)
            y_tail[n] = part[512:].reshape(extra, hid.shape[1], width)

    def hoist(j):
        span = pl.ds(pl.multiple_of(j * lane, lane), lane)
        cols = [column(cum_t[...], 2 * j + i) for i in range(2)]
        rowv = [cum_ref[pl.ds(2 * j + i, 1), :] for i in range(2)]
        steps = [column(step_t[...], 2 * j + i) for i in range(2)]
        steps_col = jnp.where(left_of, steps[0], steps[1])
        col = jnp.where(left_of, cols[0], cols[1])
        end_row = jnp.where(left_of, cols[0][row_count - 1 :], cols[1][row_count - 1 :])
        fac[:, span] = steps_col * jnp.exp(end_row - col)
        for i in range(blocks):
            lo, hi = i * block, (i + 1) * block
            if i < blocks - 1:
                fac_mid[lo:hi, span] = steps_col[lo:hi] * jnp.exp(col[hi - 1 : hi] - col[lo:hi])
            for q in range(2):
                r = rowv[q][:, lo:hi]
                w = jnp.exp(jnp.minimum(r - cols[q][lo:hi], 0.0)) * (bc[i] * steps[q][lo:hi])
                w_top, w_low = halves(w)
                mix[j, i, q * block : (q + 1) * block, :] = w_top
                mix[j, i, (2 + q) * block : (3 + q) * block, :] = w_low
                base = rowv[q][:, lo - 1 : lo] if i else jnp.zeros((1, 1), F32)
                m_top, m_low = halves(c_ref[:, lo:hi] * jnp.exp(r - base))
                lead[j, i, q * n_state : (q + 1) * n_state, :] = m_top
                lead[j, i, (2 + q) * n_state : (3 + q) * n_state, :] = m_low

    def state_step(j, _):
        span = pl.ds(pl.multiple_of(j * lane, lane), lane)
        rowv = [cum_ref[pl.ds(2 * j + q, 1), :] for q in range(2)]
        ends = [[r[:, hi - 1 : hi] for r in rowv] for hi in range(block, row_count + 1, block)]
        state = jnp.zeros((n_state, lane), F32)
        for i in reversed(range(blocks)):
            g_top, g_low = halves(inner[i * block : (i + 1) * block, span])
            x = dot(lead[j, i], jnp.concatenate([g_top, g_low], axis=1))
            x = x[:, :lane] + jnp.concatenate(
                [x[: 2 * n_state, lane:], jnp.zeros((2 * n_state, lane), F32)], axis=0
            )
            x = x[: 2 * n_state] + x[2 * n_state :]
            if i < blocks - 1:
                mid[i, :, span] = state
            edge = jnp.where(left_of, ends[i][0], ends[i][1])
            if i:
                edge = edge - jnp.where(left_of, ends[i - 1][0], ends[i - 1][1])
            state = jnp.where(left_of, x[:n_state], x[n_state:]) + jnp.exp(edge) * state
        agg[0, :, span] = state
        return 0

    def read_state(lo, hi, state):
        top, low = halves(state)
        return dot(b_wide[lo:hi, :], jnp.concatenate([top, low, top], axis=0))

    def within_step(j, _):
        span = pl.ds(pl.multiple_of(j * lane, lane), lane)
        skip = skip_ref[:, span]
        for i in range(blocks):
            lo, hi = i * block, (i + 1) * block
            g = inner[lo:hi, span]
            g_top, g_low = halves(g)
            x = dot(mix[j, i], jnp.concatenate([g_top, g_low], axis=1))
            part = []
            for q in range(2):
                top = x[q * block : (q + 1) * block]
                low = x[(2 + q) * block : (3 + q) * block]
                part.append(top[:, :lane] + top[:, lane:] + low[:, :lane])
            result = jnp.where(left_of, part[0], part[1]) + skip * g
            if i < blocks - 1:
                seen = read_state(lo, hi, mid[i, :, span])
                result += fac_mid[lo:hi, span] * seen
            inner[lo:hi, span] = result
        return 0

    def scores(u):
        i, c = u // parts, u % parts
        g = nearest(z, i)

        def one(s, _):
            total = acc[s, i]
            for half in range(2):
                part = rows[2 * u + half, s].astype(F32) * y_ref[
                    c, s * n_exp + g, :, half * half_w : (half + 1) * half_w
                ]
                for j in range(half_w // 128):
                    total = total + part[:, j * 128 : (j + 1) * 128]
            acc[s, i] = total
            return 0

        lax.fori_loop(0, n_seq, one, 0)

    low_half = lax.broadcasted_iota(jnp.int32, (2 * n_exp, width), 0) < n_exp

    def tail_scores():
        def one(p, _):
            sums = [acc_tail[p, i] for i in range(extra)]
            for c in range(parts):
                half, at = c // (parts // 2), (c % (parts // 2)) * width
                first = tail[half, 2 * p].astype(F32)[:, at : at + width]
                second = tail[half, 2 * p + 1].astype(F32)[:, at : at + width]
                even = jnp.where(low_half, first, pltpu.roll(second, n_exp, 0))
                odd = jnp.where(low_half, pltpu.roll(first, n_exp, 0), second)
                for i, part in enumerate((even, odd)):
                    first_q = pl.multiple_of(p * 2 * n_exp, 2 * n_exp)
                    part = part * y_tail[c, i, pl.ds(first_q, 2 * n_exp), :]
                    for j in range(width // 128):
                        sums[i] = sums[i] + part[:, j * 128 : (j + 1) * 128]
            for i in range(extra):
                acc_tail[p, i] = sums[i]
            return 0

        lax.fori_loop(0, n_seq // 2, one, 0)

    def choose(u, g, c):
        taken = dot(pick[g], gath[c, g]).astype(BF)
        rows[2 * u, me] = taken[:, :half_w]
        rows[2 * u + 1, me] = taken[:, half_w:]
        x_start(u, 0)

    def first_step(c, _):
        choose(c, z, c)
        return 0

    with scope("first"):
        lax.fori_loop(0, parts, first_step, 0)
        hid_copy.start()
        for k in range(parts):
            down_load(k).start()
        for k in range(parts):
            proj_load(k).start()

    def unit_step(t, _):
        i, c = t // parts, t % parts

        with scope("ztake"):
            @pl.when(i >= 1)
            def _():
                z_take(c, i)

            @pl.when(jnp.logical_and(i >= 1, i < n_exp - 1))
            def _():
                z_send(c, i)

        with scope("pick"):
            @pl.when(i >= 1)
            def _():
                choose(t, nearest(z, i), c)

        with scope("tailrows"):
            @pl.when(i == n_exp - 1)
            def _():
                left = dot(pick_tail[...], gath[c].reshape(row_count, width))
                at = pl.multiple_of((c % (parts // 2)) * width, width)
                tail[c // (parts // 2), me, :, pl.ds(at, width)] = left[: 2 * n_exp].astype(BF)

            for half in range(2):
                @pl.when(t == units - 1 - (1 - half) * (parts // 2))
                def _(half=half):
                    t_start(half, 0)

            @pl.when(t == units - 1)
            def _():
                t_pass(0, 1)

        with scope("hoist0"):
            @pl.when(jnp.logical_and(t >= 1, t <= 2))
            def _():
                for v in range(pairs // 4):
                    hoist((t - 1) * (pairs // 4) + v)

        with scope("once"):
            @pl.when(t == 0)
            def _():
                prepare()
                d_copy(0).start()
                settle()

            @pl.when(t == parts - 1)
            def _():
                hid_copy.wait()
                settled(down, load_sem.at[1])
                settled(proj, load_sem.at[2])

            for i_ in range(len(order)):
                @pl.when(t == 2 * i_ + 3)
                def _(i_=i_):
                    d_copy(i_).wait_recv()
                    if i_ + 1 < len(order):
                        span_sum[i_ + 1] = span_sum[i_] + span_got[i_]
                        d_copy(i_ + 1).start()

        with scope("project"):
            @pl.when(jnp.logical_and(t >= parts - 1, t < 3 * parts - 1))
            def _():
                project(2 * (t - parts + 1))
                project(2 * (t - parts + 1) + 1)

        with scope("inner"):
            @pl.when(i == n_exp - 1)
            def _():
                part = dot(gath[c].reshape(row_count, width), proj[c], ((1,), (1,)))

                @pl.when(c == 0)
                def _():
                    inner[...] = part

                @pl.when(c > 0)
                def _():
                    inner[...] += part

        with scope("hoist"):
            @pl.when(jnp.logical_and(t >= units - 1 - pairs // 2, t < units - 1))
            def _():
                hoist(t - (units - 1 - pairs // 2) + pairs // 2)

        with scope("score"):
            @pl.when(jnp.logical_and(t >= 3 * parts - 1, t < units - 1))
            def _():
                for v in range(2):
                    u = 2 * (t - 3 * parts + 1) + v
                    x_take(u, n_stage)
                    scores(u)

        with scope("xpass"):
            for at, todo in FIRST_STEPS.items():
                @pl.when(t == at)
                def _(todo=todo):
                    for u, stage in todo:
                        x_pass(u, stage)

            @pl.when(t > parts)
            def _():
                x_pass(t - LAG_FIRST, 1)

            @pl.when(t >= parts + LAG_SECOND)
            def _():
                x_pass(t - LAG_SECOND, 2)

        return 0

    with scope("unitloop"):
        lax.fori_loop(0, units, unit_step, 0)

    def a_copy(i):
        return pltpu.make_async_remote_copy(
            src_ref=agg.at[i],
            dst_ref=got.at[i],
            send_sem=as_sem,
            recv_sem=ar_sem.at[i],
            device_id={"seq": flip(me, order[i])},
        )

    reach = [jnp.zeros((1, channels), F32)]

    def combine(i):
        a_copy(i).wait_recv()
        low = ((me // order[i]) % 2) == 0
        other, other_t = got[i], span_got[i, 0:1, :]
        own, own_t = agg[i], span_sum[i, 0:1, :]
        added = jnp.where(low, jnp.exp(reach[0]) * other, 0.0)
        if i == 0:
            carry[...] = added
        else:
            carry[...] += added
        reach[0] = reach[0] + jnp.where(low, other_t, 0.0)
        if i + 1 < len(order):
            first = jnp.where(low, own, other)
            first_t = jnp.where(low, own_t, other_t)
            second = jnp.where(low, other, own)
            agg[i + 1] = first + jnp.exp(first_t) * second
            a_copy(i + 1).start()

    def post():
        for i in reversed(range(n_exp)):
            for apart in reversed(range(n_seq)):
                if i == 0 and apart == 0:
                    continue
                target = me
                for bit in order:
                    if apart & bit:
                        target = flip(target, bit)
                pltpu.make_async_remote_copy(
                    src_ref=mail.at[target, i // 2],
                    dst_ref=inbox.at[mine_id],
                    send_sem=ms_sem,
                    recv_sem=mr_sem,
                    device_id={"seq": target, "exp": nearest(z, i)},
                ).start()

    def finish(i):
        def one(s, _):
            both = jnp.transpose(acc[s, 2 * i : 2 * i + 2].reshape(2 * main, 128))
            mail[s, i, 0:1, :] = jnp.sum(both, axis=0, keepdims=True)
            return 0

        lax.fori_loop(0, n_seq, one, 0, unroll=True)

    done = [2 * parts]

    def count(upto):
        with scope("c%d" % upto):
            for u in range(done[0], upto):
                x_take(u, n_stage)
                scores(u)
            done[0] = max(done[0], upto)

    def within(first, last):
        with scope("within%d" % first):
            lax.fori_loop(first * pairs // 8, last * pairs // 8, within_step, 0)

    with scope("state"):
        lax.fori_loop(0, pairs, state_step, 0)
        a_copy(0).start()
    with scope("pb"):
        x_pass(units - 1, 1)
        t_pass(1, 1)
    within(0, 2)
    with scope("pc"):
        x_pass(units - 3, 2)
        t_pass(0, 2)
    with scope("comb0"):
        combine(0)
    count(units - 3)
    with scope("pc2"):
        x_pass(units - 2, 2)
    within(2, 3)
    with scope("finish0"):
        for i in range(n_exp // 2 - 1):
            finish(i)
    with scope("pd"):
        x_pass(units - 1, 2)
        t_pass(1, 2)
    count(units - 1)
    count(units)
    with scope("tailscore"):
        for half in range(2):
            t_take(half, n_stage)
        tail_scores()
    with scope("finish1"):
        finish(n_exp // 2 - 1)
        wide = jnp.transpose(acc_tail[...].reshape(n_seq // 2 * extra * 2 * n_exp, 128))
        wide = jnp.sum(wide, axis=0, keepdims=True)
        wide = jnp.concatenate([wide, jnp.zeros((1, 128 - wide.shape[1]), F32)], axis=1)
        for s in range(n_seq):
            for i in range(n_exp // 2):
                mail[s, i, 1:2, :] = wide
    with scope("post"):
        post()
        inbox[mine_id] = mail[me, 0]

    with scope("comb1"):
        combine(1)
    within(3, 8)
    with scope("comb2"):
        combine(2)
    with scope("out"):
        for i in range(blocks):
            lo, hi = i * block, (i + 1) * block
            from_carry = read_state(lo, hi, carry[...])
            out_buf[lo:hi, :] = (inner[lo:hi, :] + fac[lo:hi, :] * from_carry).astype(BF)
            pltpu.make_async_copy(
                out_buf.at[pl.ds(lo, block)], out_hbm.at[pl.ds(lo, block)], out_sem
            ).start()

    with scope("drain"):
        settled(rows.at[:, pl.ds(0, n_seq - 1)], xs_sem.at[0])
        settled(tail.at[:, pl.ds(0, n_seq - 1)], xs_sem.at[1])
        for d in range(n_exp - 1):
            z_sent(d)
        settled(agg, as_sem)
        settled(span_sum, ds_sem)
    with scope("mail"):
        settled(inbox.at[pl.ds(0, n_dev - 1)], mr_sem)
    with scope("gate"):
        for e in range(n_exp):
            total = inbox[e]
            for i in range(1, n_seq):
                total = total + inbox[i * n_exp + e]
            vals[2 * e : 2 * e + 2, :] = total
        first, rest = halves(vals[...])
        second, third = halves(vals[...] - first.astype(F32))
        split = jnp.concatenate([first, second, third, third], axis=0)
        found = dot(split, where_at[...])
        found = found[: 2 * n_exp] + found[2 * n_exp : 4 * n_exp] + found[4 * n_exp : 6 * n_exp]
        for k in range(ids_ref.shape[0]):
            named = lax.broadcasted_iota(jnp.int32, (2 * n_exp, tok), 0) == spot[k : k + 1, :]
            value = jnp.where(named, found[:, k * tok : (k + 1) * tok], 0.0)
            gate_ref[k : k + 1, :] = jnp.sum(value, axis=0, keepdims=True)
        settled(inbox.at[pl.ds(0, n_dev - 1)], ms_sem)
        pltpu.make_async_copy(out_buf, out_hbm, out_sem).wait()


def pass_on(wide_in, gate_in, wide_out, gate_out, wide, gate, come, go):
    strips = come.shape[0] - 1
    size = wide.shape[0] // strips

    def parts_of(i):
        if i == strips:
            return gate_in, gate, gate_out
        span = pl.ds(i * size, size)
        return wide_in.at[span], wide.at[span], wide_out.at[span]

    def move(i, leg):
        refs = parts_of(i)
        return pltpu.make_async_copy(refs[leg], refs[leg + 1], (come, go)[leg].at[i])

    for i in range(strips + 1):
        move(i, 0).start()
    for i in range(strips + 1):
        move(i, 0).wait()
        move(i, 1).start()
    for i in range(strips + 1):
        move(i, 1).wait()


def plan(n_seq, n_exp, tok, depth, channels, cap, hidden, state, top):
    parts = 4
    width = depth // parts
    main = cap // 16 * 16
    extra = cap - main
    row_count = n_exp * tok
    block = min(256, row_count)
    blocks = row_count // block
    heads = channels // HEAD
    pairs = heads // 2
    stages = n_seq.bit_length() - 1
    steps = n_exp - 1
    units = n_exp * parts
    groups = n_seq * n_exp
    shapes = [
        ((parts, n_exp, tok, width), BF),
        ((parts, channels, width), BF),
        ((cap, groups, hidden), BF),
        ((parts, hidden, width), BF),
        ((512 + extra * groups, hidden), BF),
        ((parts, groups, main, width), F32),
        ((parts, extra, groups, width), F32),
        ((2 * units, n_seq, main, width // 2), BF),
        ((2, n_seq, 2 * n_exp, depth // 2), BF),
        ((n_exp, main, tok), BF),
        ((16, row_count), BF),
        ((row_count, channels), F32),
        ((row_count, channels), F32),
        ((max(row_count - block, 8), channels), F32),
        ((n_seq, n_exp, main, 128), F32),
        ((n_seq // 2, extra, 2 * n_exp, 128), F32),
        ((heads, row_count), F32),
        ((row_count, heads), F32),
        ((row_count, heads), F32),
        ((row_count, state), F32),
        ((blocks, block, block), F32),
        ((pairs, blocks, 4 * block, block), BF),
        ((pairs, blocks, 4 * state, block), BF),
        ((max(blocks - 1, 1), state, channels), F32),
        ((stages, 8, channels), F32),
        ((stages, 8, channels), F32),
        ((stages, state, channels), F32),
        ((stages, state, channels), F32),
        ((state, channels), F32),
        ((8, tok), jnp.int32),
        ((n_seq, n_exp // 2, 2, 128), F32),
        ((groups, 2, 128), F32),
        ((2 * n_exp, 128), F32),
        ((row_count, channels), BF),
        ((128, top * tok), BF),
        ((heads, row_count), F32),
        ((heads, row_count), F32),
        ((state, row_count), F32),
        ((state, row_count), F32),
        ((1, channels), F32),
        ((top, row_count), jnp.int32),
        ((row_count, 3 * state), BF),
    ]
    total = 0
    for shape, kind in shapes:
        size = 1
        for extent in shape:
            size *= extent
        total += size * (2 if kind is BF else 4)
    fits = (
        total < VMEM_ROOM - (3 << 20)
        and n_seq & (n_seq - 1) == 0
        and stages == 3
        and n_exp == 4
        and groups == 32
        and main == 64
        and extra == 2
        and top == 2
        and depth % (256 * parts) == 0
        and channels % (2 * HEAD) == 0
        and pairs == 8
        and row_count % block == 0
        and tok == 128
    )
    sems = [
        (10,),
        (2, steps), (2, parts, steps),
        (2,), (units + 2, stages),
        (), (stages,), (), (stages,),
        (), (), (),
    ]
    return fits, (n_seq, n_exp, tok, cap, parts, width), shapes, sems


def quick(
    fitted, grad_out, out_proj, step_size, log_decay, b_input, c_output, skip_gain, expert_ids,
    hidden_act, w_down,
):
    _, sizes, shapes, sems = fitted
    n_seq, n_exp, tok, cap, parts, width = sizes
    vmem = pl.BlockSpec(memory_space=pltpu.VMEM)
    hbm = pl.BlockSpec(memory_space=pl.ANY)
    row_count, channels = n_exp * tok, out_proj.shape[0]
    d_inner, d_gate = pl.pallas_call(
        functools.partial(fused, sizes),
        out_shape=(
            jax.ShapeDtypeStruct((row_count, channels), BF),
            jax.ShapeDtypeStruct((expert_ids.shape[1], tok), F32),
        ),
        in_specs=[hbm] * 10,
        out_specs=(hbm, vmem),
        scratch_shapes=[pltpu.VMEM(shape, kind) for shape, kind in shapes]
        + [pltpu.SemaphoreType.DMA(s) if s else pltpu.SemaphoreType.DMA for s in sems],
        compiler_params=pltpu.CompilerParams(
            collective_id=0, has_side_effects=True, vmem_limit_bytes=VMEM_ROOM
        ),
    )(
        grad_out, out_proj, hidden_act.transpose(0, 2, 1, 3), w_down, step_size, log_decay, b_input, c_output,
        skip_gain.reshape(1, -1), expert_ids.T,
    )
    return pl.pallas_call(
        pass_on,
        out_shape=(
            jax.ShapeDtypeStruct(d_inner.shape, BF),
            jax.ShapeDtypeStruct(d_gate.shape, F32),
        ),
        in_specs=[hbm] * 2,
        out_specs=(hbm, hbm),
        scratch_shapes=[
            pltpu.VMEM(d_inner.shape, BF), pltpu.VMEM(d_gate.shape, F32),
            pltpu.SemaphoreType.DMA((5,)), pltpu.SemaphoreType.DMA((5,)),
        ],
    )(d_inner, d_gate)


def route(*args):
    grad_out, out_proj, step_size, log_decay, b_input, c_output, skip_gain, ids, hidden, down = args
    fitted = plan(
        lax.axis_size("seq"), lax.axis_size("exp"), grad_out.shape[0], grad_out.shape[1],
        out_proj.shape[0], hidden.shape[2], hidden.shape[3], b_input.shape[0], ids.shape[1],
    )
    if fitted[0]:
        return quick(fitted, *args)
    return shards(*args)


def solution(mesh):
    in_specs = (
        P(("seq", "exp"), None),
        P("exp", None),
        P("exp", "seq"),
        P("exp", "seq"),
        P(None, "seq"),
        P(None, "seq"),
        P("exp"),
        P("seq", None),
        P("exp", None, None, "seq"),
        P("exp", "seq", None),
    )
    out_specs = (P("seq", "exp"), P(None, ("seq", "exp")))
    return jax.shard_map(route, mesh=mesh, in_specs=in_specs, out_specs=out_specs, check_vma=False)
```

```python
import functools

import jax
import jax.numpy as jnp
from jax import lax
from jax.experimental import pallas as pl
from jax.experimental.pallas import tpu as pltpu
from jax.sharding import PartitionSpec as P

HEAD = 64


highest = lax.Precision.HIGHEST


def block_pass(state_in, pieces):
    grad_block, decay_block, step_block, b_block, c_block = pieces
    cum_decay = jnp.cumsum(decay_block, axis=1)
    gap_table = cum_decay[:, None, :] - cum_decay[:, :, None]
    upper_mask = lax.broadcasted_iota(jnp.int32, gap_table.shape, 2) >= lax.broadcasted_iota(
        jnp.int32, gap_table.shape, 1
    )
    weights = jnp.where(upper_mask, jnp.exp(jnp.where(upper_mask, gap_table, 0.0)), 0.0)
    intersection = lax.dot_general(
        b_block,
        c_block,
        (((0,), (0,)), ((), ())),
        precision=highest,
        preferred_element_type=jnp.float32,
    )
    within = jnp.einsum("hut,thp->uhp", weights * intersection[None], grad_block, precision=highest)
    tail_decay = jnp.exp(cum_decay[:, -1:] - cum_decay)
    from_state = (
        jnp.einsum("nu,hnp->uhp", b_block, state_in, precision=highest) * tail_decay.T[:, :, None]
    )
    result = step_block.T[:, :, None] * (within + from_state)
    state_out = jnp.einsum(
        "ht,nt,thp->hnp", jnp.exp(cum_decay), c_block, grad_block, precision=highest
    )
    state_out = state_out + jnp.exp(cum_decay[:, -1])[:, None, None] * state_in
    return (state_out, result)


def local_sweep(grad_rows, decay_rows, step_rows, b_rows, c_rows, start_state):
    row_count = grad_rows.shape[0]
    head_count = decay_rows.shape[0]
    block_len = min(512, row_count)
    block_count = row_count // block_len
    pieces = (
        grad_rows.reshape(block_count, block_len, head_count, grad_rows.shape[2]),
        decay_rows.reshape(head_count, block_count, block_len).transpose(1, 0, 2),
        step_rows.reshape(head_count, block_count, block_len).transpose(1, 0, 2),
        b_rows.reshape(b_rows.shape[0], block_count, block_len).transpose(1, 0, 2),
        c_rows.reshape(c_rows.shape[0], block_count, block_len).transpose(1, 0, 2),
    )
    state_out, results = lax.scan(block_pass, start_state, pieces, reverse=True)
    return (state_out, results.reshape(row_count, head_count, grad_rows.shape[2]))


def route_table(groups, expert, cap_len):
    hit_mask = jnp.any(groups == expert, axis=2)
    rank_ids = jnp.cumsum(hit_mask.astype(jnp.int32), axis=1) - 1
    slot_ids = lax.broadcasted_iota(jnp.int32, (1, 1, cap_len), 2)
    chosen = jnp.logical_and(hit_mask[:, :, None], rank_ids[:, :, None] == slot_ids)
    token_ids = lax.broadcasted_iota(jnp.int32, chosen.shape, 1)
    position = jnp.sum(jnp.where(chosen, token_ids, 0), axis=1)
    filled = jnp.any(chosen, axis=1)
    return (position, filled)


def slot_lookup(slot_table, own_ids, cap_len, expert_count):
    experts_iota = lax.broadcasted_iota(jnp.int32, (1, 1, expert_count), 2)
    onehot = own_ids[:, :, None] == experts_iota
    member = jnp.any(onehot, axis=1).astype(jnp.int32)
    rank_ids = jnp.cumsum(member, axis=0) - 1
    slot_of = jnp.sum(jnp.where(onehot, rank_ids[:, None, :], 0), axis=2)
    picked = jnp.sum(jnp.where(onehot[:, :, :, None], slot_table[None, None], 0.0), axis=2)
    slot_iota = lax.broadcasted_iota(jnp.int32, (1, 1, cap_len), 2)
    return jnp.sum(jnp.where(slot_of[:, :, None] == slot_iota, picked, 0.0), axis=2)


def shards(
    grad_out,
    out_proj,
    step_size,
    log_decay,
    b_input,
    c_output,
    skip_gain,
    expert_ids,
    hidden_act,
    w_down,
):
    exp_index = lax.axis_index("exp")
    seq_index = lax.axis_index("seq")
    exp_count = lax.axis_size("exp")
    seq_count = lax.axis_size("seq")
    tok_len = grad_out.shape[0]
    cap_len = hidden_act.shape[2]
    gathered = lax.all_gather(grad_out, "exp", axis=0, tiled=True)
    groups = expert_ids.reshape(exp_count, tok_len, expert_ids.shape[1])
    position, filled = route_table(groups, exp_index, cap_len)
    flat_index = (position + lax.broadcasted_iota(jnp.int32, position.shape, 0) * tok_len).reshape(
        -1
    )
    slot_rows = jnp.take(gathered, flat_index, axis=0)
    slot_rows = jnp.where(filled.reshape(-1, 1), slot_rows, jnp.zeros_like(slot_rows))
    saved_rows = hidden_act.reshape(-1, hidden_act.shape[3])
    weights = w_down[0]
    projected = lax.dot_general(
        lax.all_gather(slot_rows, "seq", axis=0, tiled=True),
        weights,
        (((1,), (1,)), ((), ())),
        preferred_element_type=jnp.float32,
    )
    partial_scores = jnp.sum(projected * saved_rows.astype(jnp.float32), axis=1)
    head_count = out_proj.shape[0] // HEAD
    inner_grad = lax.dot_general(
        gathered, out_proj, (((1,), (1,)), ((), ())), preferred_element_type=jnp.float32
    )
    row_count = inner_grad.shape[0]
    start_state = jnp.zeros((head_count, b_input.shape[0], HEAD), jnp.float32)
    summary, swept_part = local_sweep(
        inner_grad.reshape(row_count, head_count, HEAD),
        log_decay,
        step_size,
        b_input,
        c_output,
        start_state,
    )
    total_decay = jnp.sum(log_decay, axis=1)
    all_states, all_decay = (
        lax.all_gather(summary[None], "seq", axis=0, tiled=True),
        lax.all_gather(total_decay[None], "seq", axis=0, tiled=True),
    )
    shard_ids = lax.broadcasted_iota(jnp.int32, all_decay.shape, 0)
    beyond = jnp.where(shard_ids > seq_index, all_decay, 0.0)
    exponent = jnp.cumsum(beyond, axis=0) - beyond
    factor = jnp.where(
        shard_ids > seq_index, jnp.exp(jnp.where(shard_ids > seq_index, exponent, 0.0)), 0.0
    )
    incoming = jnp.sum(factor[:, :, None, None] * all_states, axis=0)
    suffix = jnp.flip(jnp.cumsum(jnp.flip(log_decay, 1), axis=1), 1) - log_decay
    from_carry = (
        jnp.einsum("nu,hnp->uhp", b_input, incoming, precision=highest)
        * jnp.exp(suffix).T[:, :, None]
    )
    combined = swept_part + step_size.T[:, :, None] * from_carry
    d_inner = (combined.reshape(row_count, -1) + skip_gain * inner_grad).astype(jnp.bfloat16)
    summed = lax.psum_scatter(
        partial_scores.reshape(seq_count, exp_count, cap_len),
        "seq",
        scatter_dimension=0,
        tiled=True,
    )
    slot_table = lax.all_to_all(
        summed.reshape(exp_count, 1, cap_len), "exp", split_axis=0, concat_axis=1, tiled=True
    ).reshape(exp_count, cap_len)
    own_ids = lax.dynamic_slice_in_dim(expert_ids, exp_index * tok_len, tok_len, 0)
    d_gate = slot_lookup(slot_table, own_ids, cap_len, exp_count).T
    return (d_inner, d_gate)


VMEM_ROOM = 63 << 20
BF = jnp.bfloat16
F32 = jnp.float32
LAG_FIRST = 1
LAG_SECOND = 3
LAG_THIRD = 5
RING = 8
scope = jax.named_scope


def halves(x):
    top = x.astype(BF)
    return top, (x - top.astype(F32)).astype(BF)


def dot(x, y, dims=((1,), (0,)), precision=None):
    return lax.dot_general(x, y, (dims, ((), ())), precision=precision, preferred_element_type=F32)


def flip(index, bit):
    return index + bit - 2 * bit * ((index // bit) % 2)


def column(table, h):
    lanes = lax.broadcasted_iota(jnp.int32, table.shape, 1)
    return jnp.sum(jnp.where(lanes == h, table, 0.0), axis=1, keepdims=True)


def nearest(z, i):
    upper = z // 2
    low = z + upper * (3 - 2 * z)
    group = i + low * (1 - i // 2) * (1 - 2 * i)
    return group + upper * (3 - 2 * group)


def turn_of(z, group):
    upper = z // 2
    low = z + upper * (3 - 2 * z)
    mirrored = group + upper * (3 - 2 * group)
    return mirrored + low * (1 - mirrored // 2) * (1 - 2 * mirrored)


def fused(
    sizes,
    grad_hbm, proj_hbm, hid_hbm, down_hbm, step_hbm, decay_hbm, b_hbm, c_hbm, skip_hbm, ids_hbm,
    out_hbm, gate_ref,
    gath, proj, hid, down, turned, y_ref, y_tail, rows, tail, pick, pick_tail, inner, fac, fac_mid,
    acc, acc_tail, cum_ref, cum_t, step_t, b_t, bc, mix, lead, mid, span_sum, span_got, agg, got,
    carry, spot, mail, inbox, vals, out_buf, where_at, step_ref, decay_ref, b_ref, c_ref, skip_ref, ids_ref, b_wide,
    load_sem,
    zs_sem, zr_sem, xs_sem, xr_sem, ds_sem, dr_sem, as_sem, ar_sem, ms_sem, mr_sem, out_sem,
):
    n_seq, n_exp, tok, cap, parts, width = sizes
    me = lax.axis_index("seq")
    z = lax.axis_index("exp")
    row_count = n_exp * tok
    n_dev = n_seq * n_exp
    mine_id = me * n_exp + z
    bits = [1 << i for i in range(1, n_seq.bit_length() - 1)]
    order = [1] + bits
    n_stage = len(bits)
    block = bc.shape[1]
    blocks = row_count // block
    channels = inner.shape[1]
    lane = 2 * HEAD
    pairs = channels // lane
    main = y_ref.shape[2]
    extra = cap - main
    half_w = width // 2
    units = n_exp * parts
    n_state = b_t.shape[1]

    def load(k):
        return pltpu.make_async_copy(
            grad_hbm.at[:, pl.ds(k * width, width)], gath.at[k, z], load_sem.at[0]
        )

    def down_load(k):
        return pltpu.make_async_copy(
            down_hbm.at[0, :, pl.ds(k * width, width)], down.at[k], load_sem.at[1]
        )

    def proj_load(k):
        return pltpu.make_async_copy(
            proj_hbm.at[:, pl.ds(k * width, width)], proj.at[k], load_sem.at[2]
        )

    hid_copy = pltpu.make_async_copy(hid_hbm.at[0], hid, load_sem.at[3])
    ids_copy = pltpu.make_async_copy(ids_hbm, ids_ref, load_sem.at[4])
    small = [
        pltpu.make_async_copy(src, dst, load_sem.at[5 + i])
        for i, (src, dst) in enumerate((
            (step_hbm, step_ref), (decay_hbm, decay_ref), (b_hbm, b_ref), (c_hbm, c_ref),
            (skip_hbm, skip_ref),
        ))
    ]
    barrier = pltpu.get_barrier_semaphore()

    with scope("greet"):
        for bit in order:
            pl.semaphore_signal(barrier, inc=1, device_id={"seq": flip(me, bit)})

        @pl.when(z > 0)
        def _():
            pl.semaphore_signal(barrier, inc=1, device_id={"exp": z - 1})

        @pl.when(z < n_exp - 1)
        def _():
            pl.semaphore_signal(barrier, inc=1, device_id={"exp": z + 1})

    with scope("prep"):
        for k in range(parts):
            load(k).start()
        ids_copy.start()
        for copy in small:
            copy.start()
        ids_copy.wait()
        hit = jnp.zeros((1, row_count), F32)
        for i in range(ids_ref.shape[0]):
            hit = jnp.maximum(hit, jnp.where(ids_ref[i : i + 1, :] == z, 1.0, 0.0))
        row_id = lax.broadcasted_iota(jnp.int32, (row_count, row_count), 0)
        col_id = lax.broadcasted_iota(jnp.int32, (row_count, row_count), 1)
        same = jnp.logical_and(row_id // tok == col_id // tok, row_id < col_id)
        before = dot(
            jnp.broadcast_to(hit, (16, row_count)).astype(BF), jnp.where(same, 1.0, 0.0).astype(BF)
        )
        rank = before[0:1].astype(jnp.int32)
        group = lax.broadcasted_iota(jnp.int32, (1, row_count), 1) // tok
        place = jnp.where(hit > 0.5, rank, -1)
        slots = lax.broadcasted_iota(jnp.int32, (main, tok), 0)
        for g in range(n_exp):
            chosen = slots == place[:, g * tok : (g + 1) * tok]
            pick[g] = jnp.where(chosen, 1.0, 0.0).astype(BF)
        over = jnp.where(place >= main, (place - main) * n_exp + group, -1)
        chosen = lax.broadcasted_iota(jnp.int32, (16, row_count), 0) == over
        pick_tail[...] = jnp.where(chosen, 1.0, 0.0).astype(BF)

    with scope("barrier"):
        sides = jnp.minimum(z, 1) + jnp.minimum(n_exp - 1 - z, 1)
        pl.semaphore_wait(barrier, len(order) + sides)

    def z_copy(side, k, d, owner, target):
        return pltpu.make_async_remote_copy(
            src_ref=gath.at[k, owner],
            dst_ref=gath.at[k, owner],
            send_sem=zs_sem.at[side, d],
            recv_sem=zr_sem.at[side, k, d],
            device_id={"exp": target},
        )

    def z_send(k, d):
        @pl.when(jnp.logical_and(z < n_exp - 1, z - d >= 0))
        def _():
            z_copy(0, k, d, z - d, z + 1).start()

        @pl.when(jnp.logical_and(z > 0, z + d < n_exp))
        def _():
            z_copy(1, k, d, z + d, z - 1).start()

    def settled(ref, sem):
        pltpu.make_async_copy(ref, ref, sem).wait()

    def z_sent(d):
        @pl.when(jnp.logical_and(z < n_exp - 1, z - d >= 0))
        def _():
            settled(gath.at[:, z], zs_sem.at[0, d])

        @pl.when(jnp.logical_and(z > 0, z + d < n_exp))
        def _():
            settled(gath.at[:, z], zs_sem.at[1, d])

    def z_take(k, d):
        @pl.when(z - d >= 0)
        def _():
            z_copy(0, k, d - 1, z - d, z).wait_recv()

        @pl.when(z + d < n_exp)
        def _():
            z_copy(1, k, d - 1, z + d, z).wait_recv()

    with scope("own"):
        settled(gath.at[:, z], load_sem.at[0])
        for k in range(parts):
            z_send(k, 0)

    def bit_of(half, stage):
        if stage == n_stage:
            return 1
        return bits[stage] if half == 0 else bits[n_stage - 1 - stage]

    def owners(half, stage):
        held = [me]
        for i in range(stage):
            held = held + [flip(owner, bit_of(half, i)) for owner in held]
        return held

    def x_start(u, stage):
        for j in range(1 << stage):
            for half in range(2):
                ref = rows.at[2 * u + half, owners(half, stage)[j]]
                pltpu.make_async_remote_copy(
                    src_ref=ref,
                    dst_ref=ref,
                    send_sem=xs_sem.at[0],
                    recv_sem=xr_sem.at[u % RING, stage],
                    device_id={"seq": flip(me, bit_of(half, stage))},
                ).start()

    def x_take(u, stage):
        settled(rows.at[pl.ds(2 * u, 2), pl.ds(0, 1 << stage)], xr_sem.at[u % RING, stage])

    def x_pass(u, stage):
        x_take(u, stage - 1)
        x_start(u, stage)

    def t_start(half, stage):
        for owner in owners(half, stage):
            ref = tail.at[half, owner]
            pltpu.make_async_remote_copy(
                src_ref=ref,
                dst_ref=ref,
                send_sem=xs_sem.at[1],
                recv_sem=xr_sem.at[RING + half, stage],
                device_id={"seq": flip(me, bit_of(half, stage))},
            ).start()

    def t_take(half, stage):
        settled(tail.at[half, pl.ds(0, 1 << stage)], xr_sem.at[RING + half, stage])

    def t_pass(half, stage):
        t_take(half, stage - 1)
        t_start(half, stage)

    def d_copy(i):
        return pltpu.make_async_remote_copy(
            src_ref=span_sum.at[i],
            dst_ref=span_got.at[i],
            send_sem=ds_sem,
            recv_sem=dr_sem.at[i],
            device_id={"seq": flip(me, order[i])},
        )

    def settle():
        own = pl.multiple_of(z * tok, tok)
        named = [ids_ref[k : k + 1, pl.ds(own, tok)] for k in range(ids_ref.shape[0])]
        expert = lax.broadcasted_iota(jnp.int32, (16, tok), 0)
        member = jnp.zeros((16, tok), F32)
        for ids in named:
            member = jnp.maximum(member, jnp.where(ids == expert, 1.0, 0.0))
        earlier = lax.broadcasted_iota(jnp.int32, (tok, tok), 0) < lax.broadcasted_iota(
            jnp.int32, (tok, tok), 1
        )
        ranks = dot(member.astype(BF), jnp.where(earlier, 1.0, 0.0).astype(BF)).astype(jnp.int32)
        for k, ids in enumerate(named):
            slot = jnp.zeros((1, tok), jnp.int32)
            shift = jnp.zeros((1, tok), jnp.int32)
            for e in range(n_exp):
                slot += jnp.where(ids == e, ranks[e : e + 1], 0)
                shift += jnp.where(ids == e, (turn_of(e, z) % 2) * main, 0)
            far = (me // 2) * 16 + (slot - main) * 2 * n_exp + (me % 2) * n_exp + z
            at = lax.broadcasted_iota(jnp.int32, (128, tok), 0) == jnp.where(
                slot < main, shift + slot, far
            )
            where_at[:, k * tok : (k + 1) * tok] = jnp.where(at, 1.0, 0.0).astype(BF)
            spot[k : k + 1, :] = ids * 2 + jnp.where(slot < main, 0, 1)

    def prepare():
        for copy in small:
            copy.wait()
        row_id = lax.broadcasted_iota(jnp.int32, (row_count, row_count), 0)
        col_id = lax.broadcasted_iota(jnp.int32, (row_count, row_count), 1)
        tri = jnp.where(row_id <= col_id, 1.0, 0.0)
        cum = dot(decay_ref[...], tri, precision=highest)
        cum_ref[...] = cum
        cum_t[...] = jnp.transpose(cum)
        step_t[...] = jnp.transpose(step_ref[...])
        b_t[...] = jnp.transpose(b_ref[...])
        b_top, b_low = halves(b_t[...])
        b_wide[...] = jnp.concatenate([b_top, b_top, b_low], axis=1)
        shape = (cum.shape[0], channels)
        own = lax.broadcasted_iota(jnp.int32, shape, 1) // HEAD == lax.broadcasted_iota(
            jnp.int32, shape, 0
        )
        end = jnp.sum(jnp.where(own, cum[:, row_count - 1 :], 0.0), axis=0, keepdims=True)
        span_sum[0] = jnp.broadcast_to(end, (8, channels))
        keep = lax.broadcasted_iota(jnp.int32, (block, block), 1) >= lax.broadcasted_iota(
            jnp.int32, (block, block), 0
        )
        for i in range(blocks):
            span = slice(i * block, (i + 1) * block)
            cross = dot(b_t[span, :], c_ref[:, span], precision=highest)
            bc[i] = jnp.where(keep, cross, 0.0)
        acc[...] = jnp.zeros_like(acc)
        acc_tail[...] = jnp.zeros_like(acc_tail)

    left_of = lax.broadcasted_iota(jnp.int32, (1, lane), 1) < HEAD
    perm_row = lax.broadcasted_iota(jnp.int32, (256, 256), 0)
    perm_col = lax.broadcasted_iota(jnp.int32, (256, 256), 1)

    jobs = parts * main * hid.shape[1] // 512

    def project(job):
        b, n = job // parts, job % parts
        q_first = pl.multiple_of((b % 2) * 16, 16)
        c_first = (b // 2) * 32

        @pl.when(n == 0)
        def _():
            swap = jnp.where(perm_col == (perm_row % 16) * 16 + perm_row // 16, 1.0, 0.0).astype(BF)
            for i in range(2):
                saved = hid[pl.ds(c_first + 16 * i, 16), pl.ds(q_first, 16), :]
                saved = saved.reshape(256, hid.shape[2])
                turned[256 * i : 256 * (i + 1), :] = dot(swap, saved).astype(BF)

            @pl.when(b == jobs // parts - 1)
            def _():
                turned[512:, :] = hid[main:cap].reshape(extra * hid.shape[1], hid.shape[2])

        def keep_part(part):
            for i in range(2):
                c_from = pl.multiple_of(c_first + 16 * i, 16)
                y_ref[n, pl.ds(q_first, 16), pl.ds(c_from, 16), :] = part[
                    256 * i : 256 * (i + 1)
                ].reshape(16, 16, width)

        @pl.when(b < jobs // parts - 1)
        def _():
            keep_part(dot(turned[:512, :], down[n]))

        @pl.when(b == jobs // parts - 1)
        def _():
            part = dot(turned[...], down[n])
            keep_part(part)
            y_tail[n] = part[512:].reshape(extra, hid.shape[1], width)

    def hoist(j):
        span = pl.ds(pl.multiple_of(j * lane, lane), lane)
        cols = [column(cum_t[...], 2 * j + i) for i in range(2)]
        rowv = [cum_ref[pl.ds(2 * j + i, 1), :] for i in range(2)]
        steps = [column(step_t[...], 2 * j + i) for i in range(2)]
        steps_col = jnp.where(left_of, steps[0], steps[1])
        col = jnp.where(left_of, cols[0], cols[1])
        end_row = jnp.where(left_of, cols[0][row_count - 1 :], cols[1][row_count - 1 :])
        fac[:, span] = steps_col * jnp.exp(end_row - col)
        for i in range(blocks):
            lo, hi = i * block, (i + 1) * block
            if i < blocks - 1:
                fac_mid[lo:hi, span] = steps_col[lo:hi] * jnp.exp(col[hi - 1 : hi] - col[lo:hi])
            for q in range(2):
                r = rowv[q][:, lo:hi]
                w = jnp.exp(jnp.minimum(r - cols[q][lo:hi], 0.0)) * (bc[i] * steps[q][lo:hi])
                w_top, w_low = halves(w)
                mix[j, i, q * block : (q + 1) * block, :] = w_top
                mix[j, i, (2 + q) * block : (3 + q) * block, :] = w_low
                base = rowv[q][:, lo - 1 : lo] if i else jnp.zeros((1, 1), F32)
                m_top, m_low = halves(c_ref[:, lo:hi] * jnp.exp(r - base))
                lead[j, i, q * n_state : (q + 1) * n_state, :] = m_top
                lead[j, i, (2 + q) * n_state : (3 + q) * n_state, :] = m_low

    def state_step(j, _):
        span = pl.ds(pl.multiple_of(j * lane, lane), lane)
        rowv = [cum_ref[pl.ds(2 * j + q, 1), :] for q in range(2)]
        ends = [[r[:, hi - 1 : hi] for r in rowv] for hi in range(block, row_count + 1, block)]
        state = jnp.zeros((n_state, lane), F32)
        for i in reversed(range(blocks)):
            g_top, g_low = halves(inner[i * block : (i + 1) * block, span])
            x = dot(lead[j, i], jnp.concatenate([g_top, g_low], axis=1))
            x = x[:, :lane] + jnp.concatenate(
                [x[: 2 * n_state, lane:], jnp.zeros((2 * n_state, lane), F32)], axis=0
            )
            x = x[: 2 * n_state] + x[2 * n_state :]
            if i < blocks - 1:
                mid[i, :, span] = state
            edge = jnp.where(left_of, ends[i][0], ends[i][1])
            if i:
                edge = edge - jnp.where(left_of, ends[i - 1][0], ends[i - 1][1])
            state = jnp.where(left_of, x[:n_state], x[n_state:]) + jnp.exp(edge) * state
        agg[0, :, span] = state
        return 0

    def read_state(lo, hi, state):
        top, low = halves(state)
        return dot(b_wide[lo:hi, :], jnp.concatenate([top, low, top], axis=0))

    def within_step(j, _):
        span = pl.ds(pl.multiple_of(j * lane, lane), lane)
        skip = skip_ref[:, span]
        for i in range(blocks):
            lo, hi = i * block, (i + 1) * block
            g = inner[lo:hi, span]
            g_top, g_low = halves(g)
            x = dot(mix[j, i], jnp.concatenate([g_top, g_low], axis=1))
            part = []
            for q in range(2):
                top = x[q * block : (q + 1) * block]
                low = x[(2 + q) * block : (3 + q) * block]
                part.append(top[:, :lane] + top[:, lane:] + low[:, :lane])
            result = jnp.where(left_of, part[0], part[1]) + skip * g
            if i < blocks - 1:
                seen = read_state(lo, hi, mid[i, :, span])
                result += fac_mid[lo:hi, span] * seen
            inner[lo:hi, span] = result
        return 0

    def scores(u):
        i, c = u // parts, u % parts
        g = nearest(z, i)

        def one(s, _):
            total = acc[s, i]
            for half in range(2):
                part = rows[2 * u + half, s].astype(F32) * y_ref[
                    c, s * n_exp + g, :, half * half_w : (half + 1) * half_w
                ]
                for j in range(half_w // 128):
                    total = total + part[:, j * 128 : (j + 1) * 128]
            acc[s, i] = total
            return 0

        lax.fori_loop(0, n_seq, one, 0)

    low_half = lax.broadcasted_iota(jnp.int32, (2 * n_exp, width), 0) < n_exp

    def tail_scores():
        def one(p, _):
            sums = [acc_tail[p, i] for i in range(extra)]
            for c in range(parts):
                half, at = c // (parts // 2), (c % (parts // 2)) * width
                first = tail[half, 2 * p].astype(F32)[:, at : at + width]
                second = tail[half, 2 * p + 1].astype(F32)[:, at : at + width]
                even = jnp.where(low_half, first, pltpu.roll(second, n_exp, 0))
                odd = jnp.where(low_half, pltpu.roll(first, n_exp, 0), second)
                for i, part in enumerate((even, odd)):
                    first_q = pl.multiple_of(p * 2 * n_exp, 2 * n_exp)
                    part = part * y_tail[c, i, pl.ds(first_q, 2 * n_exp), :]
                    for j in range(width // 128):
                        sums[i] = sums[i] + part[:, j * 128 : (j + 1) * 128]
            for i in range(extra):
                acc_tail[p, i] = sums[i]
            return 0

        lax.fori_loop(0, n_seq // 2, one, 0)

    def choose(u, g, c):
        taken = dot(pick[g], gath[c, g]).astype(BF)
        rows[2 * u, me] = taken[:, :half_w]
        rows[2 * u + 1, me] = taken[:, half_w:]
        x_start(u, 0)

    def first_step(c, _):
        choose(c, z, c)
        return 0

    with scope("first"):
        lax.fori_loop(0, parts, first_step, 0)
        hid_copy.start()
        for k in range(parts):
            down_load(k).start()
        for k in range(parts):
            proj_load(k).start()
    with scope("prepare"):
        prepare()
        d_copy(0).start()
    early = pairs // 2
    hoisted = 0
    for u in range(parts - 1):
        with scope("hoist0"):
            share = early - (parts - 2) if u == 0 else 1
            for _ in range(share):
                if hoisted < early:
                    hoist(hoisted)
                    hoisted += 1
        with scope("early%d" % u):
            x_pass(u, 1)
    for j in range(hoisted, early):
        hoist(j)

    def unit_step(t, _):
        i, c = t // parts, t % parts

        with scope("ztake"):
            z_take(c, i)

            @pl.when(i < n_exp - 1)
            def _():
                z_send(c, i)

        with scope("pick"):
            choose(t, nearest(z, i), c)

        with scope("tailrows"):
            @pl.when(i == n_exp - 1)
            def _():
                left = dot(pick_tail[...], gath[c].reshape(row_count, width))
                at = pl.multiple_of((c % (parts // 2)) * width, width)
                tail[c // (parts // 2), me, :, pl.ds(at, width)] = left[: 2 * n_exp].astype(BF)

            for half in range(2):
                @pl.when(t == units - 1 - (1 - half) * (parts // 2))
                def _(half=half):
                    t_start(half, 0)

            @pl.when(t == units - 1)
            def _():
                t_pass(0, 1)

        with scope("xsoon"):
            @pl.when(jnp.logical_and(t > 3 * parts, t < units - 1))
            def _():
                x_pass(t - LAG_FIRST, 1)

        with scope("once"):
            @pl.when(t == parts)
            def _():
                x_pass(parts - 1, 1)
                hid_copy.wait()
                settled(down, load_sem.at[1])
                settled(proj, load_sem.at[2])

            @pl.when(t == 2 * parts)
            def _():
                settle()

            for i_ in range(len(order)):
                @pl.when(t == parts + 1 + 2 * i_)
                def _(i_=i_):
                    d_copy(i_).wait_recv()
                    if i_ + 1 < len(order):
                        span_sum[i_ + 1] = span_sum[i_] + span_got[i_]
                        if i_ == 1:
                            span_sum[2, 1:2, :] = span_sum[1, 0:1, :]
                            span_sum[2, 2:3, :] = span_got[1, 0:1, :]
                        d_copy(i_ + 1).start()

        with scope("project"):
            @pl.when(t < 3 * parts)
            def _():
                project(2 * (t - parts))
                project(2 * (t - parts) + 1)

        with scope("inner"):
            @pl.when(i == n_exp - 1)
            def _():
                part = dot(gath[c].reshape(row_count, width), proj[c], ((1,), (1,)))

                @pl.when(c == 0)
                def _():
                    inner[...] = part

                @pl.when(c > 0)
                def _():
                    inner[...] += part

        with scope("hoist"):
            @pl.when(jnp.logical_and(t < 3 * parts, t % 2 == 1))
            def _():
                hoist(early + (t - parts) // 2)

        with scope("score"):
            @pl.when(jnp.logical_and(t >= 3 * parts, t < units - 1))
            def _():
                for v in range(2):
                    scores(2 * (t - 3 * parts) + v)

        with scope("xpass"):
            @pl.when(jnp.logical_and(t > parts, t <= 3 * parts))
            def _():
                x_pass(t - LAG_FIRST, 1)

            @pl.when(t == units - 1)
            def _():
                x_pass(t - LAG_FIRST, 1)

            @pl.when(t < 2 * parts)
            def _():
                x_pass(t - parts, 2)

            @pl.when(t >= parts + LAG_SECOND)
            def _():
                x_pass(t - LAG_SECOND, 2)

            @pl.when(t >= LAG_THIRD)
            def _():
                x_take(t - LAG_THIRD, n_stage)

        return 0

    with scope("unitloop"):
        lax.fori_loop(parts, units, unit_step, 0)

    reaches = [flip(me, bits[0]), flip(me, bits[1]), flip(flip(me, bits[0]), bits[1])]

    def a_copy(i):
        return pltpu.make_async_remote_copy(
            src_ref=agg.at[min(i, 1)],
            dst_ref=got.at[i],
            send_sem=as_sem.at[i],
            recv_sem=ar_sem.at[i],
            device_id={"seq": reaches[i - 1] if i else flip(me, 1)},
        )

    near_low = (me % 2) == 0
    x_low = ((me // bits[0]) % 2) == 0
    y_low = ((me // bits[1]) % 2) == 0

    def combine():
        a_copy(0).wait_recv()
        other, other_t = got[0], span_got[0, 0:1, :]
        own, own_t = agg[0], span_sum[0, 0:1, :]
        carry[...] = jnp.where(near_low, other, 0.0)
        first = jnp.where(near_low, own, other)
        first_t = jnp.where(near_low, own_t, other_t)
        second = jnp.where(near_low, other, own)
        agg[1] = first + jnp.exp(first_t) * second
        for i in (3, 2, 1):
            @pl.when(reaches[i - 1] < me)
            def _(i=i):
                a_copy(i).start()

    def combine_far():
        reach = jnp.where(near_low, span_got[0, 0:1, :], 0.0)

        @pl.when(x_low)
        def _():
            a_copy(1).wait_recv()
            carry[...] += jnp.exp(reach) * got[1]

        reach = reach + jnp.where(x_low, span_got[1, 0:1, :], 0.0)

        @pl.when(y_low)
        def _():
            a_copy(2).wait_recv()
            a_copy(3).wait_recv()
            first = jnp.where(x_low, got[2], got[3])
            first_t = jnp.where(x_low, span_got[2, 1:2, :], span_got[2, 2:3, :])
            second = jnp.where(x_low, got[3], got[2])
            carry[...] += jnp.exp(reach) * (first + jnp.exp(first_t) * second)

    def post():
        for i in reversed(range(n_exp)):
            for apart in reversed(range(n_seq)):
                if i == 0 and apart == 0:
                    continue
                target = me
                for bit in order:
                    if apart & bit:
                        target = flip(target, bit)
                pltpu.make_async_remote_copy(
                    src_ref=mail.at[target, i // 2],
                    dst_ref=inbox.at[mine_id],
                    send_sem=ms_sem,
                    recv_sem=mr_sem,
                    device_id={"seq": target, "exp": nearest(z, i)},
                ).start()

    def finish(i):
        def one(s, _):
            both = jnp.transpose(acc[s, 2 * i : 2 * i + 2].reshape(2 * main, 128))
            mail[s, i, 0:1, :] = jnp.sum(both, axis=0, keepdims=True)
            return 0

        lax.fori_loop(0, n_seq, one, 0, unroll=True)

    done = [2 * (parts - 1)]

    def count(upto):
        with scope("c%d" % upto):
            for u in range(done[0], upto):
                if u >= units - LAG_THIRD:
                    x_take(u, n_stage)
                scores(u)
            done[0] = max(done[0], upto)

    def within(first, last):
        with scope("within%d" % first):
            lax.fori_loop(first * pairs // 8, last * pairs // 8, within_step, 0)

    with scope("state"):
        lax.fori_loop(0, pairs, state_step, 0)
        a_copy(0).start()
    with scope("pb"):
        x_pass(units - 1, 1)
        t_pass(1, 1)
    with scope("comb0"):
        combine()
    within(0, 2)
    with scope("pc"):
        x_pass(units - 3, 2)
        t_pass(0, 2)
    count(units - 3)
    with scope("pc2"):
        x_pass(units - 2, 2)
    within(2, 3)
    with scope("finish0"):
        for i in range(n_exp // 2 - 1):
            finish(i)
    with scope("pd"):
        x_pass(units - 1, 2)
        t_pass(1, 2)
    count(units - 1)
    count(units)
    with scope("tailscore"):
        for half in range(2):
            t_take(half, n_stage)
        tail_scores()
    with scope("finish1"):
        finish(n_exp // 2 - 1)
        wide = jnp.transpose(acc_tail[...].reshape(n_seq // 2 * extra * 2 * n_exp, 128))
        wide = jnp.sum(wide, axis=0, keepdims=True)
        wide = jnp.concatenate([wide, jnp.zeros((1, 128 - wide.shape[1]), F32)], axis=1)
        for s in range(n_seq):
            for i in range(n_exp // 2):
                mail[s, i, 1:2, :] = wide
    with scope("post"):
        post()
        inbox[mine_id] = mail[me, 0]

    within(3, 8)
    with scope("comb2"):
        combine_far()
    with scope("out"):
        for i in range(blocks):
            lo, hi = i * block, (i + 1) * block
            from_carry = read_state(lo, hi, carry[...])
            out_buf[lo:hi, :] = (inner[lo:hi, :] + fac[lo:hi, :] * from_carry).astype(BF)
            pltpu.make_async_copy(
                out_buf.at[pl.ds(lo, block)], out_hbm.at[pl.ds(lo, block)], out_sem
            ).start()

    with scope("drain"):
        settled(rows.at[:, pl.ds(0, n_seq - 1)], xs_sem.at[0])
        settled(tail.at[:, pl.ds(0, n_seq - 1)], xs_sem.at[1])
        for d in range(n_exp - 1):
            z_sent(d)
        a_copy(0).wait_send()
        for i in (3, 2, 1):
            @pl.when(reaches[i - 1] < me)
            def _(i=i):
                a_copy(i).wait_send()

        settled(span_sum, ds_sem)
    with scope("mail"):
        settled(inbox.at[pl.ds(0, n_dev - 1)], mr_sem)
    with scope("gate"):
        for e in range(n_exp):
            total = inbox[e]
            for i in range(1, n_seq):
                total = total + inbox[i * n_exp + e]
            vals[2 * e : 2 * e + 2, :] = total
        first, rest = halves(vals[...])
        second, third = halves(vals[...] - first.astype(F32))
        split = jnp.concatenate([first, second, third, third], axis=0)
        found = dot(split, where_at[...])
        found = found[: 2 * n_exp] + found[2 * n_exp : 4 * n_exp] + found[4 * n_exp : 6 * n_exp]
        for k in range(ids_ref.shape[0]):
            named = lax.broadcasted_iota(jnp.int32, (2 * n_exp, tok), 0) == spot[k : k + 1, :]
            value = jnp.where(named, found[:, k * tok : (k + 1) * tok], 0.0)
            gate_ref[k : k + 1, :] = jnp.sum(value, axis=0, keepdims=True)
        settled(inbox.at[pl.ds(0, n_dev - 1)], ms_sem)
        pltpu.make_async_copy(out_buf, out_hbm, out_sem).wait()


def pass_on(wide_in, gate_in, wide_out, gate_out, wide, gate, come, go):
    strips = come.shape[0] - 1
    size = wide.shape[0] // strips

    def parts_of(i):
        if i == strips:
            return gate_in, gate, gate_out
        span = pl.ds(i * size, size)
        return wide_in.at[span], wide.at[span], wide_out.at[span]

    def move(i, leg):
        refs = parts_of(i)
        return pltpu.make_async_copy(refs[leg], refs[leg + 1], (come, go)[leg].at[i])

    for i in range(strips + 1):
        move(i, 0).start()
    for i in range(strips + 1):
        move(i, 0).wait()
        move(i, 1).start()
    for i in range(strips + 1):
        move(i, 1).wait()


def plan(n_seq, n_exp, tok, depth, channels, cap, hidden, state, top):
    parts = 4
    width = depth // parts
    main = cap // 16 * 16
    extra = cap - main
    row_count = n_exp * tok
    block = min(256, row_count)
    blocks = row_count // block
    heads = channels // HEAD
    pairs = heads // 2
    stages = n_seq.bit_length() - 1
    steps = n_exp - 1
    units = n_exp * parts
    groups = n_seq * n_exp
    shapes = [
        ((parts, n_exp, tok, width), BF),
        ((parts, channels, width), BF),
        ((cap, groups, hidden), BF),
        ((parts, hidden, width), BF),
        ((512 + extra * groups, hidden), BF),
        ((parts, groups, main, width), F32),
        ((parts, extra, groups, width), F32),
        ((2 * units, n_seq, main, width // 2), BF),
        ((2, n_seq, 2 * n_exp, depth // 2), BF),
        ((n_exp, main, tok), BF),
        ((16, row_count), BF),
        ((row_count, channels), F32),
        ((row_count, channels), F32),
        ((max(row_count - block, 8), channels), F32),
        ((n_seq, n_exp, main, 128), F32),
        ((n_seq // 2, extra, 2 * n_exp, 128), F32),
        ((heads, row_count), F32),
        ((row_count, heads), F32),
        ((row_count, heads), F32),
        ((row_count, state), F32),
        ((blocks, block, block), F32),
        ((pairs, blocks, 4 * block, block), BF),
        ((pairs, blocks, 4 * state, block), BF),
        ((max(blocks - 1, 1), state, channels), F32),
        ((stages, 8, channels), F32),
        ((stages, 8, channels), F32),
        ((2, state, channels), F32),
        ((stages + 1, state, channels), F32),
        ((state, channels), F32),
        ((8, tok), jnp.int32),
        ((n_seq, n_exp // 2, 2, 128), F32),
        ((groups, 2, 128), F32),
        ((2 * n_exp, 128), F32),
        ((row_count, channels), BF),
        ((128, top * tok), BF),
        ((heads, row_count), F32),
        ((heads, row_count), F32),
        ((state, row_count), F32),
        ((state, row_count), F32),
        ((1, channels), F32),
        ((top, row_count), jnp.int32),
        ((row_count, 3 * state), BF),
    ]
    total = 0
    for shape, kind in shapes:
        size = 1
        for extent in shape:
            size *= extent
        total += size * (2 if kind is BF else 4)
    fits = (
        total < VMEM_ROOM - (3 << 20)
        and n_seq & (n_seq - 1) == 0
        and stages == 3
        and n_exp == 4
        and groups == 32
        and main == 64
        and extra == 2
        and top == 2
        and depth % (256 * parts) == 0
        and channels % (2 * HEAD) == 0
        and pairs == 8
        and row_count % block == 0
        and tok == 128
    )
    sems = [
        (10,),
        (2, steps), (2, parts, steps),
        (2,), (RING + 2, stages),
        (), (stages,), (stages + 1,), (stages + 1,),
        (), (), (),
    ]
    return fits, (n_seq, n_exp, tok, cap, parts, width), shapes, sems


def quick(
    fitted, grad_out, out_proj, step_size, log_decay, b_input, c_output, skip_gain, expert_ids,
    hidden_act, w_down,
):
    _, sizes, shapes, sems = fitted
    n_seq, n_exp, tok, cap, parts, width = sizes
    vmem = pl.BlockSpec(memory_space=pltpu.VMEM)
    hbm = pl.BlockSpec(memory_space=pl.ANY)
    row_count, channels = n_exp * tok, out_proj.shape[0]
    d_inner, d_gate = pl.pallas_call(
        functools.partial(fused, sizes),
        out_shape=(
            jax.ShapeDtypeStruct((row_count, channels), BF),
            jax.ShapeDtypeStruct((expert_ids.shape[1], tok), F32),
        ),
        in_specs=[hbm] * 10,
        out_specs=(hbm, vmem),
        scratch_shapes=[pltpu.VMEM(shape, kind) for shape, kind in shapes]
        + [pltpu.SemaphoreType.DMA(s) if s else pltpu.SemaphoreType.DMA for s in sems],
        compiler_params=pltpu.CompilerParams(
            collective_id=0, has_side_effects=True, vmem_limit_bytes=VMEM_ROOM
        ),
    )(
        grad_out, out_proj, hidden_act.transpose(0, 2, 1, 3), w_down, step_size, log_decay, b_input, c_output,
        skip_gain.reshape(1, -1), expert_ids.T,
    )
    return pl.pallas_call(
        pass_on,
        out_shape=(
            jax.ShapeDtypeStruct(d_inner.shape, BF),
            jax.ShapeDtypeStruct(d_gate.shape, F32),
        ),
        in_specs=[hbm] * 2,
        out_specs=(hbm, hbm),
        scratch_shapes=[
            pltpu.VMEM(d_inner.shape, BF), pltpu.VMEM(d_gate.shape, F32),
            pltpu.SemaphoreType.DMA((5,)), pltpu.SemaphoreType.DMA((5,)),
        ],
    )(d_inner, d_gate)


def route(*args):
    grad_out, out_proj, step_size, log_decay, b_input, c_output, skip_gain, ids, hidden, down = args
    fitted = plan(
        lax.axis_size("seq"), lax.axis_size("exp"), grad_out.shape[0], grad_out.shape[1],
        out_proj.shape[0], hidden.shape[2], hidden.shape[3], b_input.shape[0], ids.shape[1],
    )
    if fitted[0]:
        return quick(fitted, *args)
    return shards(*args)


def solution(mesh):
    in_specs = (
        P(("seq", "exp"), None),
        P("exp", None),
        P("exp", "seq"),
        P("exp", "seq"),
        P(None, "seq"),
        P(None, "seq"),
        P("exp"),
        P("seq", None),
        P("exp", None, None, "seq"),
        P("exp", "seq", None),
    )
    out_specs = (P("seq", "exp"), P(None, ("seq", "exp")))
    return jax.shard_map(route, mesh=mesh, in_specs=in_specs, out_specs=out_specs, check_vma=False)
```

```python
import functools

import jax
import jax.numpy as jnp
from jax import lax
from jax.experimental import pallas as pl
from jax.experimental.pallas import tpu as pltpu
from jax.sharding import PartitionSpec as P

HEAD = 64


highest = lax.Precision.HIGHEST


def block_pass(state_in, pieces):
    grad_block, decay_block, step_block, b_block, c_block = pieces
    cum_decay = jnp.cumsum(decay_block, axis=1)
    gap_table = cum_decay[:, None, :] - cum_decay[:, :, None]
    upper_mask = lax.broadcasted_iota(jnp.int32, gap_table.shape, 2) >= lax.broadcasted_iota(
        jnp.int32, gap_table.shape, 1
    )
    weights = jnp.where(upper_mask, jnp.exp(jnp.where(upper_mask, gap_table, 0.0)), 0.0)
    intersection = lax.dot_general(
        b_block,
        c_block,
        (((0,), (0,)), ((), ())),
        precision=highest,
        preferred_element_type=jnp.float32,
    )
    within = jnp.einsum("hut,thp->uhp", weights * intersection[None], grad_block, precision=highest)
    tail_decay = jnp.exp(cum_decay[:, -1:] - cum_decay)
    from_state = (
        jnp.einsum("nu,hnp->uhp", b_block, state_in, precision=highest) * tail_decay.T[:, :, None]
    )
    result = step_block.T[:, :, None] * (within + from_state)
    state_out = jnp.einsum(
        "ht,nt,thp->hnp", jnp.exp(cum_decay), c_block, grad_block, precision=highest
    )
    state_out = state_out + jnp.exp(cum_decay[:, -1])[:, None, None] * state_in
    return (state_out, result)


def local_sweep(grad_rows, decay_rows, step_rows, b_rows, c_rows, start_state):
    row_count = grad_rows.shape[0]
    head_count = decay_rows.shape[0]
    block_len = min(512, row_count)
    block_count = row_count // block_len
    pieces = (
        grad_rows.reshape(block_count, block_len, head_count, grad_rows.shape[2]),
        decay_rows.reshape(head_count, block_count, block_len).transpose(1, 0, 2),
        step_rows.reshape(head_count, block_count, block_len).transpose(1, 0, 2),
        b_rows.reshape(b_rows.shape[0], block_count, block_len).transpose(1, 0, 2),
        c_rows.reshape(c_rows.shape[0], block_count, block_len).transpose(1, 0, 2),
    )
    state_out, results = lax.scan(block_pass, start_state, pieces, reverse=True)
    return (state_out, results.reshape(row_count, head_count, grad_rows.shape[2]))


def route_table(groups, expert, cap_len):
    hit_mask = jnp.any(groups == expert, axis=2)
    rank_ids = jnp.cumsum(hit_mask.astype(jnp.int32), axis=1) - 1
    slot_ids = lax.broadcasted_iota(jnp.int32, (1, 1, cap_len), 2)
    chosen = jnp.logical_and(hit_mask[:, :, None], rank_ids[:, :, None] == slot_ids)
    token_ids = lax.broadcasted_iota(jnp.int32, chosen.shape, 1)
    position = jnp.sum(jnp.where(chosen, token_ids, 0), axis=1)
    filled = jnp.any(chosen, axis=1)
    return (position, filled)


def slot_lookup(slot_table, own_ids, cap_len, expert_count):
    experts_iota = lax.broadcasted_iota(jnp.int32, (1, 1, expert_count), 2)
    onehot = own_ids[:, :, None] == experts_iota
    member = jnp.any(onehot, axis=1).astype(jnp.int32)
    rank_ids = jnp.cumsum(member, axis=0) - 1
    slot_of = jnp.sum(jnp.where(onehot, rank_ids[:, None, :], 0), axis=2)
    picked = jnp.sum(jnp.where(onehot[:, :, :, None], slot_table[None, None], 0.0), axis=2)
    slot_iota = lax.broadcasted_iota(jnp.int32, (1, 1, cap_len), 2)
    return jnp.sum(jnp.where(slot_of[:, :, None] == slot_iota, picked, 0.0), axis=2)


def shards(
    grad_out,
    out_proj,
    step_size,
    log_decay,
    b_input,
    c_output,
    skip_gain,
    expert_ids,
    hidden_act,
    w_down,
):
    exp_index = lax.axis_index("exp")
    seq_index = lax.axis_index("seq")
    exp_count = lax.axis_size("exp")
    seq_count = lax.axis_size("seq")
    tok_len = grad_out.shape[0]
    cap_len = hidden_act.shape[2]
    gathered = lax.all_gather(grad_out, "exp", axis=0, tiled=True)
    groups = expert_ids.reshape(exp_count, tok_len, expert_ids.shape[1])
    position, filled = route_table(groups, exp_index, cap_len)
    flat_index = (position + lax.broadcasted_iota(jnp.int32, position.shape, 0) * tok_len).reshape(
        -1
    )
    slot_rows = jnp.take(gathered, flat_index, axis=0)
    slot_rows = jnp.where(filled.reshape(-1, 1), slot_rows, jnp.zeros_like(slot_rows))
    saved_rows = hidden_act.reshape(-1, hidden_act.shape[3])
    weights = w_down[0]
    projected = lax.dot_general(
        lax.all_gather(slot_rows, "seq", axis=0, tiled=True),
        weights,
        (((1,), (1,)), ((), ())),
        preferred_element_type=jnp.float32,
    )
    partial_scores = jnp.sum(projected * saved_rows.astype(jnp.float32), axis=1)
    head_count = out_proj.shape[0] // HEAD
    inner_grad = lax.dot_general(
        gathered, out_proj, (((1,), (1,)), ((), ())), preferred_element_type=jnp.float32
    )
    row_count = inner_grad.shape[0]
    start_state = jnp.zeros((head_count, b_input.shape[0], HEAD), jnp.float32)
    summary, swept_part = local_sweep(
        inner_grad.reshape(row_count, head_count, HEAD),
        log_decay,
        step_size,
        b_input,
        c_output,
        start_state,
    )
    total_decay = jnp.sum(log_decay, axis=1)
    all_states, all_decay = (
        lax.all_gather(summary[None], "seq", axis=0, tiled=True),
        lax.all_gather(total_decay[None], "seq", axis=0, tiled=True),
    )
    shard_ids = lax.broadcasted_iota(jnp.int32, all_decay.shape, 0)
    beyond = jnp.where(shard_ids > seq_index, all_decay, 0.0)
    exponent = jnp.cumsum(beyond, axis=0) - beyond
    factor = jnp.where(
        shard_ids > seq_index, jnp.exp(jnp.where(shard_ids > seq_index, exponent, 0.0)), 0.0
    )
    incoming = jnp.sum(factor[:, :, None, None] * all_states, axis=0)
    suffix = jnp.flip(jnp.cumsum(jnp.flip(log_decay, 1), axis=1), 1) - log_decay
    from_carry = (
        jnp.einsum("nu,hnp->uhp", b_input, incoming, precision=highest)
        * jnp.exp(suffix).T[:, :, None]
    )
    combined = swept_part + step_size.T[:, :, None] * from_carry
    d_inner = (combined.reshape(row_count, -1) + skip_gain * inner_grad).astype(jnp.bfloat16)
    summed = lax.psum_scatter(
        partial_scores.reshape(seq_count, exp_count, cap_len),
        "seq",
        scatter_dimension=0,
        tiled=True,
    )
    slot_table = lax.all_to_all(
        summed.reshape(exp_count, 1, cap_len), "exp", split_axis=0, concat_axis=1, tiled=True
    ).reshape(exp_count, cap_len)
    own_ids = lax.dynamic_slice_in_dim(expert_ids, exp_index * tok_len, tok_len, 0)
    d_gate = slot_lookup(slot_table, own_ids, cap_len, exp_count).T
    return (d_inner, d_gate)


VMEM_ROOM = 63 << 20
BF = jnp.bfloat16
F32 = jnp.float32
LAG_FIRST = 1
LAG_SECOND = 3
LAG_THIRD = 5
RING = 8
scope = jax.named_scope


def halves(x):
    top = x.astype(BF)
    return top, (x - top.astype(F32)).astype(BF)


def dot(x, y, dims=((1,), (0,)), precision=None):
    return lax.dot_general(x, y, (dims, ((), ())), precision=precision, preferred_element_type=F32)


def flip(index, bit):
    return index + bit - 2 * bit * ((index // bit) % 2)


def column(table, h):
    lanes = lax.broadcasted_iota(jnp.int32, table.shape, 1)
    return jnp.sum(jnp.where(lanes == h, table, 0.0), axis=1, keepdims=True)


def nearest(z, i):
    upper = z // 2
    low = z + upper * (3 - 2 * z)
    group = i + low * (1 - i // 2) * (1 - 2 * i)
    return group + upper * (3 - 2 * group)


def turn_of(z, group):
    upper = z // 2
    low = z + upper * (3 - 2 * z)
    mirrored = group + upper * (3 - 2 * group)
    return mirrored + low * (1 - mirrored // 2) * (1 - 2 * mirrored)


def fused(
    sizes,
    grad_hbm, proj_hbm, hid_hbm, down_hbm, step_hbm, decay_hbm, b_hbm, c_hbm, skip_hbm, ids_hbm,
    out_hbm, gate_ref,
    gath, proj, hid, down, turned, y_ref, y_tail, rows, tail, pick, pick_tail, inner, fac, fac_mid,
    acc, acc_tail, cum_ref, cum_t, step_t, b_t, bc, mix, lead, mid, span_sum, span_got, agg, got,
    carry, spot, mail, inbox, vals, out_buf, where_at, step_ref, decay_ref, b_ref, c_ref, skip_ref, ids_ref, b_wide,
    load_sem,
    zs_sem, zr_sem, xs_sem, xr_sem, ds_sem, dr_sem, as_sem, ar_sem, ms_sem, mr_sem, out_sem,
):
    n_seq, n_exp, tok, cap, parts, width = sizes
    me = lax.axis_index("seq")
    z = lax.axis_index("exp")
    row_count = n_exp * tok
    n_dev = n_seq * n_exp
    mine_id = me * n_exp + z
    bits = [1 << i for i in range(1, n_seq.bit_length() - 1)]
    order = [1] + bits
    n_stage = len(bits)
    block = bc.shape[1]
    blocks = row_count // block
    channels = inner.shape[1]
    lane = 2 * HEAD
    pairs = channels // lane
    main = y_ref.shape[2]
    extra = cap - main
    half_w = width // 2
    units = n_exp * parts
    n_state = b_t.shape[1]

    def load(k):
        return pltpu.make_async_copy(
            grad_hbm.at[:, pl.ds(k * width, width)], gath.at[k, z], load_sem.at[0]
        )

    def down_load(k):
        return pltpu.make_async_copy(
            down_hbm.at[0, :, pl.ds(k * width, width)], down.at[k], load_sem.at[1]
        )

    def proj_load(k):
        return pltpu.make_async_copy(
            proj_hbm.at[:, pl.ds(k * width, width)], proj.at[k], load_sem.at[2]
        )

    hid_copy = pltpu.make_async_copy(hid_hbm.at[0], hid, load_sem.at[3])
    ids_copy = pltpu.make_async_copy(ids_hbm, ids_ref, load_sem.at[4])
    small = [
        pltpu.make_async_copy(src, dst, load_sem.at[5 + i])
        for i, (src, dst) in enumerate((
            (step_hbm, step_ref), (decay_hbm, decay_ref), (b_hbm, b_ref), (c_hbm, c_ref),
            (skip_hbm, skip_ref),
        ))
    ]
    barrier = pltpu.get_barrier_semaphore()

    with scope("greet"):
        for bit in order:
            pl.semaphore_signal(barrier, inc=1, device_id={"seq": flip(me, bit)})

        @pl.when(z > 0)
        def _():
            pl.semaphore_signal(barrier, inc=1, device_id={"exp": z - 1})

        @pl.when(z < n_exp - 1)
        def _():
            pl.semaphore_signal(barrier, inc=1, device_id={"exp": z + 1})

    with scope("prep"):
        for k in range(parts):
            load(k).start()
        ids_copy.start()
        for copy in small:
            copy.start()
        ids_copy.wait()
        hit = jnp.zeros((1, row_count), F32)
        for i in range(ids_ref.shape[0]):
            hit = jnp.maximum(hit, jnp.where(ids_ref[i : i + 1, :] == z, 1.0, 0.0))
        row_id = lax.broadcasted_iota(jnp.int32, (row_count, row_count), 0)
        col_id = lax.broadcasted_iota(jnp.int32, (row_count, row_count), 1)
        same = jnp.logical_and(row_id // tok == col_id // tok, row_id < col_id)
        before = dot(
            jnp.broadcast_to(hit, (16, row_count)).astype(BF), jnp.where(same, 1.0, 0.0).astype(BF)
        )
        rank = before[0:1].astype(jnp.int32)
        group = lax.broadcasted_iota(jnp.int32, (1, row_count), 1) // tok
        place = jnp.where(hit > 0.5, rank, -1)
        slots = lax.broadcasted_iota(jnp.int32, (main, tok), 0)
        for g in range(n_exp):
            chosen = slots == place[:, g * tok : (g + 1) * tok]
            pick[g] = jnp.where(chosen, 1.0, 0.0).astype(BF)
        over = jnp.where(place >= main, (place - main) * n_exp + group, -1)
        chosen = lax.broadcasted_iota(jnp.int32, (16, row_count), 0) == over
        pick_tail[...] = jnp.where(chosen, 1.0, 0.0).astype(BF)

    with scope("barrier"):
        sides = jnp.minimum(z, 1) + jnp.minimum(n_exp - 1 - z, 1)
        pl.semaphore_wait(barrier, len(order) + sides)

    def z_copy(side, k, d, owner, target):
        return pltpu.make_async_remote_copy(
            src_ref=gath.at[k, owner],
            dst_ref=gath.at[k, owner],
            send_sem=zs_sem.at[side, d],
            recv_sem=zr_sem.at[side, k, d],
            device_id={"exp": target},
        )

    def z_send(k, d):
        @pl.when(jnp.logical_and(z < n_exp - 1, z - d >= 0))
        def _():
            z_copy(0, k, d, z - d, z + 1).start()

        @pl.when(jnp.logical_and(z > 0, z + d < n_exp))
        def _():
            z_copy(1, k, d, z + d, z - 1).start()

    def settled(ref, sem):
        pltpu.make_async_copy(ref, ref, sem).wait()

    def z_sent(d):
        @pl.when(jnp.logical_and(z < n_exp - 1, z - d >= 0))
        def _():
            settled(gath.at[:, z], zs_sem.at[0, d])

        @pl.when(jnp.logical_and(z > 0, z + d < n_exp))
        def _():
            settled(gath.at[:, z], zs_sem.at[1, d])

    def z_take(k, d):
        @pl.when(z - d >= 0)
        def _():
            z_copy(0, k, d - 1, z - d, z).wait_recv()

        @pl.when(z + d < n_exp)
        def _():
            z_copy(1, k, d - 1, z + d, z).wait_recv()

    with scope("own"):
        settled(gath.at[:, z], load_sem.at[0])
        for k in range(parts):
            z_send(k, 0)

    def bit_of(half, stage):
        if stage == n_stage:
            return 1
        return bits[stage] if half == 0 else bits[n_stage - 1 - stage]

    def owners(half, stage):
        held = [me]
        for i in range(stage):
            held = held + [flip(owner, bit_of(half, i)) for owner in held]
        return held

    def x_start(u, stage):
        for j in range(1 << stage):
            for half in range(2):
                ref = rows.at[2 * u + half, owners(half, stage)[j]]
                pltpu.make_async_remote_copy(
                    src_ref=ref,
                    dst_ref=ref,
                    send_sem=xs_sem.at[0],
                    recv_sem=xr_sem.at[u % RING, stage],
                    device_id={"seq": flip(me, bit_of(half, stage))},
                ).start()

    def x_take(u, stage):
        settled(rows.at[pl.ds(2 * u, 2), pl.ds(0, 1 << stage)], xr_sem.at[u % RING, stage])

    def x_pass(u, stage):
        x_take(u, stage - 1)
        x_start(u, stage)

    def t_start(half, stage):
        for owner in owners(half, stage):
            ref = tail.at[half, owner]
            pltpu.make_async_remote_copy(
                src_ref=ref,
                dst_ref=ref,
                send_sem=xs_sem.at[1],
                recv_sem=xr_sem.at[RING + half, stage],
                device_id={"seq": flip(me, bit_of(half, stage))},
            ).start()

    def t_take(half, stage):
        settled(tail.at[half, pl.ds(0, 1 << stage)], xr_sem.at[RING + half, stage])

    def t_pass(half, stage):
        t_take(half, stage - 1)
        t_start(half, stage)

    def d_copy(i):
        return pltpu.make_async_remote_copy(
            src_ref=span_sum.at[i],
            dst_ref=span_got.at[i],
            send_sem=ds_sem,
            recv_sem=dr_sem.at[i],
            device_id={"seq": flip(me, order[i])},
        )

    def settle():
        own = pl.multiple_of(z * tok, tok)
        named = [ids_ref[k : k + 1, pl.ds(own, tok)] for k in range(ids_ref.shape[0])]
        expert = lax.broadcasted_iota(jnp.int32, (16, tok), 0)
        member = jnp.zeros((16, tok), F32)
        for ids in named:
            member = jnp.maximum(member, jnp.where(ids == expert, 1.0, 0.0))
        earlier = lax.broadcasted_iota(jnp.int32, (tok, tok), 0) < lax.broadcasted_iota(
            jnp.int32, (tok, tok), 1
        )
        ranks = dot(member.astype(BF), jnp.where(earlier, 1.0, 0.0).astype(BF)).astype(jnp.int32)
        for k, ids in enumerate(named):
            slot = jnp.zeros((1, tok), jnp.int32)
            shift = jnp.zeros((1, tok), jnp.int32)
            for e in range(n_exp):
                slot += jnp.where(ids == e, ranks[e : e + 1], 0)
                shift += jnp.where(ids == e, (turn_of(e, z) % 2) * main, 0)
            far = (me // 2) * 16 + (slot - main) * 2 * n_exp + (me % 2) * n_exp + z
            at = lax.broadcasted_iota(jnp.int32, (128, tok), 0) == jnp.where(
                slot < main, shift + slot, far
            )
            where_at[:, k * tok : (k + 1) * tok] = jnp.where(at, 1.0, 0.0).astype(BF)
            spot[k : k + 1, :] = ids * 2 + jnp.where(slot < main, 0, 1)

    def prepare():
        for copy in small:
            copy.wait()
        row_id = lax.broadcasted_iota(jnp.int32, (row_count, row_count), 0)
        col_id = lax.broadcasted_iota(jnp.int32, (row_count, row_count), 1)
        tri = jnp.where(row_id <= col_id, 1.0, 0.0)
        cum = dot(decay_ref[...], tri, precision=highest)
        cum_ref[...] = cum
        cum_t[...] = jnp.transpose(cum)
        step_t[...] = jnp.transpose(step_ref[...])
        b_t[...] = jnp.transpose(b_ref[...])
        b_top, b_low = halves(b_t[...])
        b_wide[...] = jnp.concatenate([b_top, b_top, b_low], axis=1)
        shape = (cum.shape[0], channels)
        own = lax.broadcasted_iota(jnp.int32, shape, 1) // HEAD == lax.broadcasted_iota(
            jnp.int32, shape, 0
        )
        end = jnp.sum(jnp.where(own, cum[:, row_count - 1 :], 0.0), axis=0, keepdims=True)
        span_sum[0] = jnp.broadcast_to(end, (8, channels))
        keep = lax.broadcasted_iota(jnp.int32, (block, block), 1) >= lax.broadcasted_iota(
            jnp.int32, (block, block), 0
        )
        for i in range(blocks):
            span = slice(i * block, (i + 1) * block)
            cross = dot(b_t[span, :], c_ref[:, span], precision=highest)
            bc[i] = jnp.where(keep, cross, 0.0)
        acc[...] = jnp.zeros_like(acc)
        acc_tail[...] = jnp.zeros_like(acc_tail)

    left_of = lax.broadcasted_iota(jnp.int32, (1, lane), 1) < HEAD
    perm_row = lax.broadcasted_iota(jnp.int32, (256, 256), 0)
    perm_col = lax.broadcasted_iota(jnp.int32, (256, 256), 1)

    jobs = parts * main * hid.shape[1] // 512

    def project(job):
        b, n = job // parts, job % parts
        q_first = pl.multiple_of((b % 2) * 16, 16)
        c_first = (b // 2) * 32

        @pl.when(n == 0)
        def _():
            swap = jnp.where(perm_col == (perm_row % 16) * 16 + perm_row // 16, 1.0, 0.0).astype(BF)
            for i in range(2):
                saved = hid[pl.ds(c_first + 16 * i, 16), pl.ds(q_first, 16), :]
                saved = saved.reshape(256, hid.shape[2])
                turned[256 * i : 256 * (i + 1), :] = dot(swap, saved).astype(BF)

            @pl.when(b == jobs // parts - 1)
            def _():
                turned[512:, :] = hid[main:cap].reshape(extra * hid.shape[1], hid.shape[2])

        def keep_part(part):
            for i in range(2):
                c_from = pl.multiple_of(c_first + 16 * i, 16)
                y_ref[n, pl.ds(q_first, 16), pl.ds(c_from, 16), :] = part[
                    256 * i : 256 * (i + 1)
                ].reshape(16, 16, width)

        @pl.when(b < jobs // parts - 1)
        def _():
            keep_part(dot(turned[:512, :], down[n]))

        @pl.when(b == jobs // parts - 1)
        def _():
            part = dot(turned[...], down[n])
            keep_part(part)
            y_tail[n] = part[512:].reshape(extra, hid.shape[1], width)

    def hoist(j):
        span = pl.ds(pl.multiple_of(j * lane, lane), lane)
        cols = [column(cum_t[...], 2 * j + i) for i in range(2)]
        rowv = [cum_ref[pl.ds(2 * j + i, 1), :] for i in range(2)]
        steps = [column(step_t[...], 2 * j + i) for i in range(2)]
        steps_col = jnp.where(left_of, steps[0], steps[1])
        col = jnp.where(left_of, cols[0], cols[1])
        end_row = jnp.where(left_of, cols[0][row_count - 1 :], cols[1][row_count - 1 :])
        fac[:, span] = steps_col * jnp.exp(end_row - col)
        for i in range(blocks):
            lo, hi = i * block, (i + 1) * block
            if i < blocks - 1:
                fac_mid[lo:hi, span] = steps_col[lo:hi] * jnp.exp(col[hi - 1 : hi] - col[lo:hi])
            for q in range(2):
                r = rowv[q][:, lo:hi]
                w = jnp.exp(jnp.minimum(r - cols[q][lo:hi], 0.0)) * (bc[i] * steps[q][lo:hi])
                w_top, w_low = halves(w)
                mix[j, i, q * block : (q + 1) * block, :] = w_top
                mix[j, i, (2 + q) * block : (3 + q) * block, :] = w_low
                base = rowv[q][:, lo - 1 : lo] if i else jnp.zeros((1, 1), F32)
                m_top, m_low = halves(c_ref[:, lo:hi] * jnp.exp(r - base))
                lead[j, i, q * n_state : (q + 1) * n_state, :] = m_top
                lead[j, i, (2 + q) * n_state : (3 + q) * n_state, :] = m_low

    def state_step(j, _):
        span = pl.ds(pl.multiple_of(j * lane, lane), lane)
        rowv = [cum_ref[pl.ds(2 * j + q, 1), :] for q in range(2)]
        ends = [[r[:, hi - 1 : hi] for r in rowv] for hi in range(block, row_count + 1, block)]
        state = jnp.zeros((n_state, lane), F32)
        for i in reversed(range(blocks)):
            g_top, g_low = halves(inner[i * block : (i + 1) * block, span])
            x = dot(lead[j, i], jnp.concatenate([g_top, g_low], axis=1))
            x = x[:, :lane] + jnp.concatenate(
                [x[: 2 * n_state, lane:], jnp.zeros((2 * n_state, lane), F32)], axis=0
            )
            x = x[: 2 * n_state] + x[2 * n_state :]
            if i < blocks - 1:
                mid[i, :, span] = state
            edge = jnp.where(left_of, ends[i][0], ends[i][1])
            if i:
                edge = edge - jnp.where(left_of, ends[i - 1][0], ends[i - 1][1])
            state = jnp.where(left_of, x[:n_state], x[n_state:]) + jnp.exp(edge) * state
        agg[0, :, span] = state
        return 0

    def read_state(lo, hi, state):
        top, low = halves(state)
        return dot(b_wide[lo:hi, :], jnp.concatenate([top, low, top], axis=0))

    def within_step(j, _):
        span = pl.ds(pl.multiple_of(j * lane, lane), lane)
        skip = skip_ref[:, span]
        for i in range(blocks):
            lo, hi = i * block, (i + 1) * block
            g = inner[lo:hi, span]
            g_top, g_low = halves(g)
            x = dot(mix[j, i], jnp.concatenate([g_top, g_low], axis=1))
            part = []
            for q in range(2):
                top = x[q * block : (q + 1) * block]
                low = x[(2 + q) * block : (3 + q) * block]
                part.append(top[:, :lane] + top[:, lane:] + low[:, :lane])
            result = jnp.where(left_of, part[0], part[1]) + skip * g
            if i < blocks - 1:
                seen = read_state(lo, hi, mid[i, :, span])
                result += fac_mid[lo:hi, span] * seen
            inner[lo:hi, span] = result
        return 0

    def scores(u):
        i, c = u // parts, u % parts
        g = nearest(z, i)

        def one(s, _):
            total = acc[s, i]
            for half in range(2):
                part = rows[2 * u + half, s].astype(F32) * y_ref[
                    c, s * n_exp + g, :, half * half_w : (half + 1) * half_w
                ]
                for j in range(half_w // 128):
                    total = total + part[:, j * 128 : (j + 1) * 128]
            acc[s, i] = total
            return 0

        lax.fori_loop(0, n_seq, one, 0)

    low_half = lax.broadcasted_iota(jnp.int32, (2 * n_exp, width), 0) < n_exp

    def tail_scores():
        def one(p, _):
            sums = [acc_tail[p, i] for i in range(extra)]
            for c in range(parts):
                half, at = c // (parts // 2), (c % (parts // 2)) * width
                first = tail[half, 2 * p].astype(F32)[:, at : at + width]
                second = tail[half, 2 * p + 1].astype(F32)[:, at : at + width]
                even = jnp.where(low_half, first, pltpu.roll(second, n_exp, 0))
                odd = jnp.where(low_half, pltpu.roll(first, n_exp, 0), second)
                for i, part in enumerate((even, odd)):
                    first_q = pl.multiple_of(p * 2 * n_exp, 2 * n_exp)
                    part = part * y_tail[c, i, pl.ds(first_q, 2 * n_exp), :]
                    for j in range(width // 128):
                        sums[i] = sums[i] + part[:, j * 128 : (j + 1) * 128]
            for i in range(extra):
                acc_tail[p, i] = sums[i]
            return 0

        lax.fori_loop(0, n_seq // 2, one, 0)

    def choose(u, g, c):
        taken = dot(pick[g], gath[c, g]).astype(BF)
        rows[2 * u, me] = taken[:, :half_w]
        rows[2 * u + 1, me] = taken[:, half_w:]
        x_start(u, 0)

    def first_step(c, _):
        choose(c, z, c)
        return 0

    with scope("first"):
        lax.fori_loop(0, parts, first_step, 0)
        hid_copy.start()
        for k in range(parts):
            down_load(k).start()
        for k in range(parts):
            proj_load(k).start()
    with scope("prepare"):
        prepare()
        d_copy(0).start()
    early = pairs // 2
    hoisted = 0
    for u in range(parts - 1):
        with scope("hoist0"):
            share = early - (parts - 2) if u == 0 else 1
            for _ in range(share):
                if hoisted < early:
                    hoist(hoisted)
                    hoisted += 1
        with scope("early%d" % u):
            x_pass(u, 1)
    for j in range(hoisted, early):
        hoist(j)

    def unit_step(t, _):
        i, c = t // parts, t % parts

        with scope("ztake"):
            z_take(c, i)

            @pl.when(i < n_exp - 1)
            def _():
                z_send(c, i)

        with scope("pick"):
            choose(t, nearest(z, i), c)

        with scope("tailrows"):
            @pl.when(i == n_exp - 1)
            def _():
                left = dot(pick_tail[...], gath[c].reshape(row_count, width))
                at = pl.multiple_of((c % (parts // 2)) * width, width)
                tail[c // (parts // 2), me, :, pl.ds(at, width)] = left[: 2 * n_exp].astype(BF)

            for half in range(2):
                @pl.when(t == units - 1 - (1 - half) * (parts // 2))
                def _(half=half):
                    t_start(half, 0)

            @pl.when(t == units - 1)
            def _():
                t_pass(0, 1)

        with scope("xsoon"):
            @pl.when(jnp.logical_and(t > 3 * parts, t < units - 1))
            def _():
                x_pass(t - LAG_FIRST, 1)

        with scope("once"):
            @pl.when(t == parts)
            def _():
                x_pass(parts - 1, 1)
                hid_copy.wait()
                settled(down, load_sem.at[1])
                settled(proj, load_sem.at[2])

            @pl.when(t == 2 * parts)
            def _():
                settle()

            for i_ in range(len(order)):
                @pl.when(t == parts + 1 + 2 * i_)
                def _(i_=i_):
                    d_copy(i_).wait_recv()
                    if i_ + 1 < len(order):
                        span_sum[i_ + 1] = span_sum[i_] + span_got[i_]
                        if i_ == 1:
                            span_sum[2, 1:2, :] = span_sum[1, 0:1, :]
                            span_sum[2, 2:3, :] = span_got[1, 0:1, :]
                        d_copy(i_ + 1).start()

        with scope("project"):
            @pl.when(t < 3 * parts)
            def _():
                project(2 * (t - parts))
                project(2 * (t - parts) + 1)

        with scope("inner"):
            @pl.when(i == n_exp - 1)
            def _():
                part = dot(gath[c].reshape(row_count, width), proj[c], ((1,), (1,)))

                @pl.when(c == 0)
                def _():
                    inner[...] = part

                @pl.when(c > 0)
                def _():
                    inner[...] += part

        with scope("hoist"):
            @pl.when(jnp.logical_and(t < 3 * parts, t % 2 == 1))
            def _():
                hoist(early + (t - parts) // 2)

        with scope("score"):
            @pl.when(jnp.logical_and(t >= 3 * parts, t < units - 1))
            def _():
                for v in range(2):
                    scores(2 * (t - 3 * parts) + v)

        with scope("xpass"):
            @pl.when(jnp.logical_and(t > parts, t <= 3 * parts))
            def _():
                x_pass(t - LAG_FIRST, 1)

            @pl.when(t == units - 1)
            def _():
                x_pass(t - LAG_FIRST, 1)

            @pl.when(t < 2 * parts)
            def _():
                x_pass(t - parts, 2)

            @pl.when(t >= parts + LAG_SECOND)
            def _():
                x_pass(t - LAG_SECOND, 2)

            @pl.when(t >= LAG_THIRD)
            def _():
                x_take(t - LAG_THIRD, n_stage)

        return 0

    with scope("unitloop"):
        lax.fori_loop(parts, units, unit_step, 0)

    reaches = [flip(me, bits[0]), flip(me, bits[1]), flip(flip(me, bits[0]), bits[1])]

    def a_copy(i):
        return pltpu.make_async_remote_copy(
            src_ref=agg.at[min(i, 1)],
            dst_ref=got.at[i],
            send_sem=as_sem.at[i],
            recv_sem=ar_sem.at[i],
            device_id={"seq": reaches[i - 1] if i else flip(me, 1)},
        )

    near_low = (me % 2) == 0
    x_low = ((me // bits[0]) % 2) == 0
    y_low = ((me // bits[1]) % 2) == 0

    def combine():
        a_copy(0).wait_recv()
        other, other_t = got[0], span_got[0, 0:1, :]
        own, own_t = agg[0], span_sum[0, 0:1, :]
        carry[...] = jnp.where(near_low, other, 0.0)
        first = jnp.where(near_low, own, other)
        first_t = jnp.where(near_low, own_t, other_t)
        second = jnp.where(near_low, other, own)
        agg[1] = first + jnp.exp(first_t) * second
        for i in (3, 2, 1):
            @pl.when(reaches[i - 1] < me)
            def _(i=i):
                a_copy(i).start()

    def combine_far():
        reach = jnp.where(near_low, span_got[0, 0:1, :], 0.0)

        @pl.when(x_low)
        def _():
            a_copy(1).wait_recv()
            carry[...] += jnp.exp(reach) * got[1]

        reach = reach + jnp.where(x_low, span_got[1, 0:1, :], 0.0)

        @pl.when(y_low)
        def _():
            a_copy(2).wait_recv()
            a_copy(3).wait_recv()
            first = jnp.where(x_low, got[2], got[3])
            first_t = jnp.where(x_low, span_got[2, 1:2, :], span_got[2, 2:3, :])
            second = jnp.where(x_low, got[3], got[2])
            carry[...] += jnp.exp(reach) * (first + jnp.exp(first_t) * second)

    def post():
        for i in reversed(range(n_exp)):
            for apart in reversed(range(n_seq)):
                if i == 0 and apart == 0:
                    continue
                target = me
                for bit in order:
                    if apart & bit:
                        target = flip(target, bit)
                pltpu.make_async_remote_copy(
                    src_ref=mail.at[target, i // 2],
                    dst_ref=inbox.at[mine_id],
                    send_sem=ms_sem,
                    recv_sem=mr_sem,
                    device_id={"seq": target, "exp": nearest(z, i)},
                ).start()

    def finish(i):
        def one(s, _):
            both = jnp.transpose(acc[s, 2 * i : 2 * i + 2].reshape(2 * main, 128))
            mail[s, i, 0:1, :] = jnp.sum(both, axis=0, keepdims=True)
            return 0

        lax.fori_loop(0, n_seq, one, 0, unroll=True)

    done = [2 * (parts - 1)]

    def count(upto):
        with scope("c%d" % upto):
            for u in range(done[0], upto):
                if u >= units - LAG_THIRD:
                    x_take(u, n_stage)
                scores(u)
            done[0] = max(done[0], upto)

    def within(first, last):
        with scope("within%d" % first):
            lax.fori_loop(first * pairs // 8, last * pairs // 8, within_step, 0)

    with scope("state"):
        lax.fori_loop(0, pairs, state_step, 0)
        a_copy(0).start()
    with scope("pb"):
        x_pass(units - 1, 1)
        t_pass(1, 1)
    with scope("comb0"):
        combine()
    within(0, 2)
    with scope("pc"):
        x_pass(units - 3, 2)
        t_pass(0, 2)
    count(units - 3)
    with scope("pc2"):
        x_pass(units - 2, 2)
    within(2, 3)
    with scope("finish0"):
        for i in range(n_exp // 2 - 1):
            finish(i)
    count(units - 2)
    with scope("pd"):
        t_pass(1, 2)
        x_pass(units - 1, 2)
    count(units - 1)
    count(units)
    with scope("tailscore"):
        for half in range(2):
            t_take(half, n_stage)
        tail_scores()
    with scope("finish1"):
        finish(n_exp // 2 - 1)
        wide = jnp.transpose(acc_tail[...].reshape(n_seq // 2 * extra * 2 * n_exp, 128))
        wide = jnp.sum(wide, axis=0, keepdims=True)
        wide = jnp.concatenate([wide, jnp.zeros((1, 128 - wide.shape[1]), F32)], axis=1)
        for s in range(n_seq):
            for i in range(n_exp // 2):
                mail[s, i, 1:2, :] = wide
    with scope("post"):
        post()
        inbox[mine_id] = mail[me, 0]

    within(3, 8)
    with scope("comb2"):
        combine_far()
    with scope("out"):
        for i in range(blocks):
            lo, hi = i * block, (i + 1) * block
            from_carry = read_state(lo, hi, carry[...])
            out_buf[lo:hi, :] = (inner[lo:hi, :] + fac[lo:hi, :] * from_carry).astype(BF)
            pltpu.make_async_copy(
                out_buf.at[pl.ds(lo, block)], out_hbm.at[pl.ds(lo, block)], out_sem
            ).start()

    with scope("drain"):
        settled(rows.at[:, pl.ds(0, n_seq - 1)], xs_sem.at[0])
        settled(tail.at[:, pl.ds(0, n_seq - 1)], xs_sem.at[1])
        for d in range(n_exp - 1):
            z_sent(d)
        a_copy(0).wait_send()
        for i in (3, 2, 1):
            @pl.when(reaches[i - 1] < me)
            def _(i=i):
                a_copy(i).wait_send()

        settled(span_sum, ds_sem)
    with scope("mail"):
        settled(inbox.at[pl.ds(0, n_dev - 1)], mr_sem)
    with scope("gate"):
        for e in range(n_exp):
            total = inbox[e]
            for i in range(1, n_seq):
                total = total + inbox[i * n_exp + e]
            vals[2 * e : 2 * e + 2, :] = total
        first, rest = halves(vals[...])
        second, third = halves(vals[...] - first.astype(F32))
        split = jnp.concatenate([first, second, third, third], axis=0)
        found = dot(split, where_at[...])
        found = found[: 2 * n_exp] + found[2 * n_exp : 4 * n_exp] + found[4 * n_exp : 6 * n_exp]
        for k in range(ids_ref.shape[0]):
            named = lax.broadcasted_iota(jnp.int32, (2 * n_exp, tok), 0) == spot[k : k + 1, :]
            value = jnp.where(named, found[:, k * tok : (k + 1) * tok], 0.0)
            gate_ref[k : k + 1, :] = jnp.sum(value, axis=0, keepdims=True)
        settled(inbox.at[pl.ds(0, n_dev - 1)], ms_sem)
        pltpu.make_async_copy(out_buf, out_hbm, out_sem).wait()


def pass_on(wide_in, gate_in, wide_out, gate_out, wide, gate, come, go):
    strips = come.shape[0] - 1
    size = wide.shape[0] // strips

    def parts_of(i):
        if i == strips:
            return gate_in, gate, gate_out
        span = pl.ds(i * size, size)
        return wide_in.at[span], wide.at[span], wide_out.at[span]

    def move(i, leg):
        refs = parts_of(i)
        return pltpu.make_async_copy(refs[leg], refs[leg + 1], (come, go)[leg].at[i])

    for i in range(strips + 1):
        move(i, 0).start()
    for i in range(strips + 1):
        move(i, 0).wait()
        move(i, 1).start()
    for i in range(strips + 1):
        move(i, 1).wait()


def plan(n_seq, n_exp, tok, depth, channels, cap, hidden, state, top):
    parts = 4
    width = depth // parts
    main = cap // 16 * 16
    extra = cap - main
    row_count = n_exp * tok
    block = min(256, row_count)
    blocks = row_count // block
    heads = channels // HEAD
    pairs = heads // 2
    stages = n_seq.bit_length() - 1
    steps = n_exp - 1
    units = n_exp * parts
    groups = n_seq * n_exp
    shapes = [
        ((parts, n_exp, tok, width), BF),
        ((parts, channels, width), BF),
        ((cap, groups, hidden), BF),
        ((parts, hidden, width), BF),
        ((512 + extra * groups, hidden), BF),
        ((parts, groups, main, width), F32),
        ((parts, extra, groups, width), F32),
        ((2 * units, n_seq, main, width // 2), BF),
        ((2, n_seq, 2 * n_exp, depth // 2), BF),
        ((n_exp, main, tok), BF),
        ((16, row_count), BF),
        ((row_count, channels), F32),
        ((row_count, channels), F32),
        ((max(row_count - block, 8), channels), F32),
        ((n_seq, n_exp, main, 128), F32),
        ((n_seq // 2, extra, 2 * n_exp, 128), F32),
        ((heads, row_count), F32),
        ((row_count, heads), F32),
        ((row_count, heads), F32),
        ((row_count, state), F32),
        ((blocks, block, block), F32),
        ((pairs, blocks, 4 * block, block), BF),
        ((pairs, blocks, 4 * state, block), BF),
        ((max(blocks - 1, 1), state, channels), F32),
        ((stages, 8, channels), F32),
        ((stages, 8, channels), F32),
        ((2, state, channels), F32),
        ((stages + 1, state, channels), F32),
        ((state, channels), F32),
        ((8, tok), jnp.int32),
        ((n_seq, n_exp // 2, 2, 128), F32),
        ((groups, 2, 128), F32),
        ((2 * n_exp, 128), F32),
        ((row_count, channels), BF),
        ((128, top * tok), BF),
        ((heads, row_count), F32),
        ((heads, row_count), F32),
        ((state, row_count), F32),
        ((state, row_count), F32),
        ((1, channels), F32),
        ((top, row_count), jnp.int32),
        ((row_count, 3 * state), BF),
    ]
    total = 0
    for shape, kind in shapes:
        size = 1
        for extent in shape:
            size *= extent
        total += size * (2 if kind is BF else 4)
    fits = (
        total < VMEM_ROOM - (3 << 20)
        and n_seq & (n_seq - 1) == 0
        and stages == 3
        and n_exp == 4
        and groups == 32
        and main == 64
        and extra == 2
        and top == 2
        and depth % (256 * parts) == 0
        and channels % (2 * HEAD) == 0
        and pairs == 8
        and row_count % block == 0
        and tok == 128
    )
    sems = [
        (10,),
        (2, steps), (2, parts, steps),
        (2,), (RING + 2, stages),
        (), (stages,), (stages + 1,), (stages + 1,),
        (), (), (),
    ]
    return fits, (n_seq, n_exp, tok, cap, parts, width), shapes, sems


def quick(
    fitted, grad_out, out_proj, step_size, log_decay, b_input, c_output, skip_gain, expert_ids,
    hidden_act, w_down,
):
    _, sizes, shapes, sems = fitted
    n_seq, n_exp, tok, cap, parts, width = sizes
    vmem = pl.BlockSpec(memory_space=pltpu.VMEM)
    hbm = pl.BlockSpec(memory_space=pl.ANY)
    row_count, channels = n_exp * tok, out_proj.shape[0]
    d_inner, d_gate = pl.pallas_call(
        functools.partial(fused, sizes),
        out_shape=(
            jax.ShapeDtypeStruct((row_count, channels), BF),
            jax.ShapeDtypeStruct((expert_ids.shape[1], tok), F32),
        ),
        in_specs=[hbm] * 10,
        out_specs=(hbm, vmem),
        scratch_shapes=[pltpu.VMEM(shape, kind) for shape, kind in shapes]
        + [pltpu.SemaphoreType.DMA(s) if s else pltpu.SemaphoreType.DMA for s in sems],
        compiler_params=pltpu.CompilerParams(
            collective_id=0, has_side_effects=True, vmem_limit_bytes=VMEM_ROOM
        ),
    )(
        grad_out, out_proj, hidden_act.transpose(0, 2, 1, 3), w_down, step_size, log_decay, b_input, c_output,
        skip_gain.reshape(1, -1), expert_ids.T,
    )
    return pl.pallas_call(
        pass_on,
        out_shape=(
            jax.ShapeDtypeStruct(d_inner.shape, BF),
            jax.ShapeDtypeStruct(d_gate.shape, F32),
        ),
        in_specs=[hbm] * 2,
        out_specs=(hbm, hbm),
        scratch_shapes=[
            pltpu.VMEM(d_inner.shape, BF), pltpu.VMEM(d_gate.shape, F32),
            pltpu.SemaphoreType.DMA((5,)), pltpu.SemaphoreType.DMA((5,)),
        ],
    )(d_inner, d_gate)


def route(*args):
    grad_out, out_proj, step_size, log_decay, b_input, c_output, skip_gain, ids, hidden, down = args
    fitted = plan(
        lax.axis_size("seq"), lax.axis_size("exp"), grad_out.shape[0], grad_out.shape[1],
        out_proj.shape[0], hidden.shape[2], hidden.shape[3], b_input.shape[0], ids.shape[1],
    )
    if fitted[0]:
        return quick(fitted, *args)
    return shards(*args)


def solution(mesh):
    in_specs = (
        P(("seq", "exp"), None),
        P("exp", None),
        P("exp", "seq"),
        P("exp", "seq"),
        P(None, "seq"),
        P(None, "seq"),
        P("exp"),
        P("seq", None),
        P("exp", None, None, "seq"),
        P("exp", "seq", None),
    )
    out_specs = (P("seq", "exp"), P(None, ("seq", "exp")))
    return jax.shard_map(route, mesh=mesh, in_specs=in_specs, out_specs=out_specs, check_vma=False)
```
